32 devices in a mesh: dp: 8 (over y, x, core), mp: 4 (over z).
Axes of the slice: x: 2, y: 2, z: 4, core: 2. Of those that a mesh axis runs over, the one named last changes fastest.
Arguments:
- tokens: bfloat16 [8192, 2048], P('dp'), may hold values from -6 to 6
- cotangent: bfloat16 [8192, 2048], P('dp'), may hold values from -6 to 6
- counts: int32 [8], replicated, may hold values from 1 to 1024, 5120 in all
- w_qkv: bfloat16 [2048, 3, 2048], P('dp', None, 'mp'), may hold values from -0.125 to 0.125
- w_out: bfloat16 [2048, 2048], P('mp', 'dp'), may hold values from -1 to 1
- w_fc1: bfloat16 [2048, 8192], P('dp', 'mp'), may hold values from -0.125 to 0.125
- w_fc2: bfloat16 [8192, 2048], P('mp', 'dp'), may hold values from -0.0625 to 0.0625
- ln1_gain: bfloat16 [2048], P('dp'), may hold values from 0.5 to 1.5
- ln1_bias: bfloat16 [2048], P('dp'), may hold values from -1.796875 to 1.796875
- ln2_gain: bfloat16 [2048], P('dp'), may hold values from 0.5 to 1.5
- ln2_bias: bfloat16 [2048], P('dp'), may hold values from -1.796875 to 1.796875
- qv_bias: bfloat16 [2, 2048], P(None, ('mp', 'dp')), may hold values from -1.796875 to 1.796875
- out_bias: bfloat16 [2048], P('dp'), may hold values from -1.796875 to 1.796875
- fc1_bias: bfloat16 [8192], P(('mp', 'dp')), may hold values from -1.796875 to 1.796875
- fc2_bias: bfloat16 [2048], P('dp'), may hold values from -1.796875 to 1.796875
Outputs:
- out_tokens: bfloat16 [8192, 2048], P('dp')
- grad_tokens: float32 [8192, 2048], P('dp')
- grad_w_qkv: float32 [2048, 3, 2048], P('dp', None, 'mp')
- grad_w_out: float32 [2048, 2048], P('mp', 'dp')
- grad_w_fc1: float32 [2048, 8192], P('dp', 'mp')
- grad_w_fc2: float32 [8192, 2048], P('mp', 'dp')
- grad_ln1_gain: float32 [2048], P('dp')
- grad_ln1_bias: float32 [2048], P('dp')
- grad_ln2_gain: float32 [2048], P('dp')
- grad_ln2_bias: float32 [2048], P('dp')
- grad_qv_bias: float32 [2, 2048], P(None, ('mp', 'dp'))
- grad_out_bias: float32 [2048], P('dp')
- grad_fc1_bias: float32 [8192], P(('mp', 'dp'))
- grad_fc2_bias: float32 [2048], P('dp')
The draws below stay inside these ranges and needn't reach their ends.
Inputs may be any that keep to these rules, and one draw needn't show every extreme that they name: counts[g] is the number of live tokens of group g's sequence, at the start of its 1024 slots; the largest count equals 1024.
All inputs are finite; a program needn't handle non-finite values.
Results may differ from the reference program's by a relative error of at most 0.014.
Values may be sent and summed in bfloat16 or wider, within the bound.
A program may use at most 192 MiB of HBM per device.

```python
import math
import jax
import jax.numpy as jnp
import numpy as np
from jax import lax

D = 2048
HEADS = 16
HEAD = 128
FF = 8192
SEQ = 1024
GROUPS = 8
TOKENS = 8192
N_DP = 8


def with_spikes(entries, key, source, target, blocks, factor):
    def block_of(axis_at):
        return (jnp.arange(entries.shape[axis_at]) // (entries.shape[axis_at] // blocks)).reshape((-1,) + (1,) * (entries.ndim - 1 - axis_at))

    one_side = jax.random.permutation(key, blocks)[block_of(target)]
    second = (block_of(target) + blocks // 2) % blocks
    return jnp.where((block_of(source) == one_side) | (block_of(source) == second), factor * entries, entries)


def shard_levels(key, shape, split, smallest, high):
    def one(axis_at, blocks):
        heights = jax.random.uniform(jax.random.fold_in(jax.random.fold_in(key, 6), axis_at), (blocks,), jnp.float32, smallest / len(split), high / len(split))
        return jnp.repeat(jnp.exp(heights), shape[axis_at] // blocks).reshape((-1,) + (1,) * (len(shape) - axis_at - 1))

    gain = one(*split[0])
    for cut in split[1:]:
        gain = gain * one(*cut)
    return gain


def length_profile(count, total, reach, skew):
    portions = [(1 << 20) // math.isqrt(standing ** skew) + 1 for standing in range(2, count + 1)]
    rest, given = total - reach - (count - 1), [1] * (count - 1)
    while rest > 0:
        free = [i for i in range(count - 1) if given[i] < reach]
        mass, left = sum([portions[i] for i in free]), rest
        for i in free:
            extra = min(reach - given[i], max(1, left * portions[i] // mass), rest)
            given[i] = given[i] + extra
            rest = rest - extra
    return np.array([reach] + given)


def uneven(key, amount, total, limit, lean):
    if amount == 2:
        one = jax.random.randint(key, (), max(1, total - limit), min(limit, total - 1) + 1)
        return jnp.stack([one, total - one])
    sizes = jnp.asarray(length_profile(amount, total, limit, lean), jnp.int32)
    couples = (amount - 1) // 2
    source_of, sink = sizes[1:1 + 2 * couples:2], sizes[2:2 + 2 * couples:2]
    room = jnp.minimum(source_of - 1, limit - sink)
    moved = jax.random.randint(jax.random.fold_in(key, 1), (couples,), 0, 1 << 20) % (room + 1)
    sizes = sizes.at[1:1 + 2 * couples:2].set(source_of - moved).at[2:2 + 2 * couples:2].set(sink + moved)
    return sizes[jax.random.permutation(jax.random.fold_in(key, 2), amount)]


def gaussian(key, shape, scale, limit, split=(), kind=jnp.bfloat16):
    values = jax.random.normal(key, shape, jnp.float32) * scale
    if len(split) > 0:
        values = shard_levels(key, shape, split, -0.22, 0.18) * values
    return jnp.clip(values, min=-limit, max=limit).astype(kind)


def bell_draw_with(key, extent, scale, limit, cuts, heavy, kind=jnp.bfloat16):
    result = scale * jax.random.normal(key, extent, jnp.float32)
    if cuts:
        result = result * shard_levels(key, extent, cuts, -0.22, 0.18)
    return jnp.clip(with_spikes(result, jax.random.fold_in(key, 3), *heavy), -limit, limit).astype(kind)


def setup_inputs(seed: int = 0) -> dict:
    splits = jax.random.split(jax.random.key(seed), 16)
    return {
        "tokens": gaussian(splits[0], (TOKENS, D), 1.0, 6.0, ((0, 8),)),
        "cotangent": bell_draw_with(splits[1], (TOKENS, D), 1.0, 6.0, ((0, 8),), (0, 1, 8, 2.0)),
        "counts": uneven(splits[2], GROUPS, N_DP * SEQ * 5 // 8, SEQ, 2).astype(jnp.int32),
        "w_qkv": gaussian(splits[3], (D, 3, D), D ** -0.5, 0.125, ((0, 8), (2, 4))),
        "w_out": gaussian(splits[4], (D, D), (D // 64) ** -0.5, 1.0, ((0, 4), (1, 8))),
        "w_fc1": gaussian(splits[5], (D, FF), D ** -0.5, 0.125, ((0, 8), (1, 4))),
        "w_fc2": gaussian(splits[6], (FF, D), FF ** -0.5, 0.0625, ((0, 4), (1, 8))),
        "ln1_gain": jnp.clip(1.0 + 0.1 * jax.random.normal(splits[7], (D,), jnp.float32), 0.5, 1.5).astype(jnp.bfloat16),
        "ln1_bias": gaussian(splits[8], (D,), 0.3, 1.796875, ((0, 8),)),
        "ln2_gain": jnp.clip(1.0 + 0.1 * jax.random.normal(splits[9], (D,), jnp.float32), 0.5, 1.5).astype(jnp.bfloat16),
        "ln2_bias": gaussian(splits[10], (D,), 0.3, 1.796875, ((0, 8),)),
        "qv_bias": gaussian(splits[11], (2, D), 0.3, 1.796875, ((1, 32),)),
        "out_bias": gaussian(splits[12], (D,), 0.3, 1.796875, ((0, 8),)),
        "fc1_bias": gaussian(splits[13], (FF,), 0.3, 1.796875, ((0, 32),)),
        "fc2_bias": gaussian(splits[14], (D,), 0.3, 1.796875, ((0, 8),)),
    }


EPS = 1e-05
NEG = -1e+30
HIGH = lax.Precision.HIGHEST

@jax.custom_vjp
def low(v):
    return lax.optimization_barrier(v.astype(jnp.bfloat16)).astype(jnp.float32)

@jax.custom_vjp
def low_back(v):
    return v

def low_keep(v):
    return (low(v), None)

def low_pass(kept, grad):
    return (grad,)

def back_keep(v):
    return (v, None)

def back_low(kept, grad):
    return (low(grad),)
low.defvjp(low_keep, low_pass)
low_back.defvjp(back_keep, back_low)

def layer_norm(values, gain_vec, shift_vec):
    center = values - lax.optimization_barrier(jnp.mean(values, axis=-1, keepdims=True))
    spread = lax.optimization_barrier(jnp.mean(center * center, axis=-1, keepdims=True))
    return center * lax.rsqrt(spread + EPS) * gain_vec + shift_vec

def forward(inputs, w_qkv, w_out, w_fc1, w_fc2, gain_one, shift_one, gain_two, shift_two, bias_qv, bias_out, bias_fc1, bias_fc2):
    seq_rows = inputs.shape[0]
    inv_root = 1.0 / math.sqrt(HEAD)
    normed_one = low(layer_norm(inputs, gain_one, shift_one))
    projected = low_back(jnp.einsum('sd,dce->sce', normed_one, w_qkv, precision=HIGH))
    queries = low(projected[:, 0] + bias_qv[0]).reshape(seq_rows, HEADS, HEAD)
    key_heads = low(projected[:, 1]).reshape(seq_rows, HEADS, HEAD)
    values = low(projected[:, 2] + bias_qv[1]).reshape(seq_rows, HEADS, HEAD)
    raw_scores = low_back(jnp.einsum('qhd,khd->hqk', queries, key_heads, precision=HIGH) * inv_root)
    future = lax.broadcasted_iota(jnp.int32, (seq_rows, seq_rows), 1) > lax.broadcasted_iota(jnp.int32, (seq_rows, seq_rows), 0)
    scores = jnp.where(future[None], NEG, raw_scores)
    row_peak = lax.optimization_barrier(jnp.max(scores, axis=-1, keepdims=True))
    exp_terms = jnp.exp(scores - row_peak)
    prob_low = low(exp_terms / lax.optimization_barrier(jnp.sum(exp_terms, axis=-1, keepdims=True)))
    mixed_heads = low(low_back(jnp.einsum('hqk,khd->qhd', prob_low, values, precision=HIGH))).reshape(seq_rows, D)
    residual = inputs + (low_back(jnp.dot(mixed_heads, w_out, precision=HIGH)) + bias_out)
    normed_two = low(layer_norm(residual, gain_two, shift_two))
    preact = low_back(jnp.dot(normed_two, w_fc1, precision=HIGH)) + bias_fc1
    activated = low(jax.nn.gelu(preact, approximate=True))
    return residual + (low_back(jnp.dot(activated, w_fc2, precision=HIGH)) + bias_fc2)

def reference(tokens, cotangent, counts, w_qkv, w_out, w_fc1, w_fc2, ln1_gain, ln1_bias, ln2_gain, ln2_bias, qv_bias, out_bias, fc1_bias, fc2_bias):
    params = tuple((param.astype(jnp.float32) for param in (w_qkv, w_out, w_fc1, w_fc2, ln1_gain, ln1_bias, ln2_gain, ln2_bias, qv_bias, out_bias, fc1_bias, fc2_bias)))
    seq_tokens = tokens.reshape(N_DP, SEQ, D)
    seq_cots = cotangent.reshape(N_DP, SEQ, D)
    total_count = jnp.sum(counts).astype(jnp.float32)

    def one_group(running_sums, group_items):
        group_tokens, group_cot, own_count = group_items
        produced, pullback = jax.vjp(forward, group_tokens.astype(jnp.float32), *params)
        live_rows = lax.iota(jnp.int32, SEQ) < own_count
        grad_out = jnp.where(live_rows[:, None], group_cot.astype(jnp.float32), jnp.zeros((), jnp.float32))
        pulled = pullback(grad_out)
        weight_share = own_count.astype(jnp.float32) / total_count
        running_sums = tuple((summed + weight_share * gradient for summed, gradient in zip(running_sums, pulled[1:])))
        return (running_sums, (produced.astype(jnp.bfloat16), pulled[0]))
    zero_grads = tuple((jnp.zeros_like(param) for param in params))
    running, (produced_all, input_grads) = lax.scan(one_group, zero_grads, (seq_tokens, seq_cots, counts))
    return (produced_all.reshape(TOKENS, D), input_grads.reshape(TOKENS, D).astype(jnp.float32), running[0], running[1], running[2], running[3], running[4], running[5], running[6], running[7], running[8], running[9], running[10], running[11])
```

```python
import math

import jax
import jax.numpy as jnp
from jax import lax
from jax.sharding import PartitionSpec as P

HEAD = 128


EPS = 1e-05
NEG = -1e30


def layer_norm(values, gain_vec, shift_vec):
    center = values - jnp.mean(values, axis=-1, keepdims=True)
    spread = jnp.mean(center * center, axis=-1, keepdims=True)
    return center * lax.rsqrt(spread + EPS) * gain_vec + shift_vec


def smooth_gate(values):
    return jax.nn.gelu(values, approximate=True)


def causal_scores(queries, key_heads, inv_root):
    row_count = queries.shape[0]
    raw_scores = (
        jnp.einsum("qhd,khd->hqk", queries, key_heads, preferred_element_type=jnp.float32)
        * inv_root
    )
    future = lax.broadcasted_iota(jnp.int32, (row_count, row_count), 1) > lax.broadcasted_iota(
        jnp.int32, (row_count, row_count), 0
    )
    return jnp.where(future[None], NEG, raw_scores)


def shards(
    tokens,
    cotangent,
    counts,
    w_qkv,
    w_out,
    w_fc1,
    w_fc2,
    ln1_gain,
    ln1_bias,
    ln2_gain,
    ln2_bias,
    qv_bias,
    out_bias,
    fc1_bias,
    fc2_bias,
):
    whole_qkv = lax.all_gather(w_qkv, "dp", axis=0, tiled=True)
    whole_out = lax.all_gather(w_out, "dp", axis=1, tiled=True)
    whole_fc1 = lax.all_gather(w_fc1, "dp", axis=0, tiled=True)
    whole_fc2 = lax.all_gather(w_fc2, "dp", axis=1, tiled=True)
    vectors = (
        ln1_gain,
        ln1_bias,
        ln2_gain,
        ln2_bias,
        out_bias,
        fc2_bias,
        fc1_bias,
        qv_bias.reshape(-1),
    )
    packed = lax.all_gather(jnp.concatenate(vectors), "dp", axis=0).astype(jnp.float32)
    wide = []
    at = 0
    for vector in vectors:
        wide.append(packed[:, at : at + vector.shape[0]])
        at += vector.shape[0]
    gain_one, shift_one, gain_two, shift_two, bias_out, bias_fc2, bias_fc1 = (
        part.reshape(-1) for part in wide[:7]
    )
    n_dp = packed.shape[0]
    bias_qv = wide[7].reshape(n_dp, 2, -1).transpose(1, 0, 2).reshape(2, -1)
    seq_rows = tokens.shape[0]
    local_width = whole_qkv.shape[2]
    heads_here = local_width // HEAD
    inv_root = 1.0 / math.sqrt(HEAD)
    inputs = tokens.astype(jnp.float32)
    normed_one = layer_norm(inputs, gain_one, shift_one).astype(jnp.bfloat16)
    projected = jnp.einsum("sd,dce->sce", normed_one, whole_qkv, preferred_element_type=jnp.float32)
    queries = (
        (projected[:, 0] + bias_qv[0]).astype(jnp.bfloat16).reshape(seq_rows, heads_here, HEAD)
    )
    key_heads = projected[:, 1].astype(jnp.bfloat16).reshape(seq_rows, heads_here, HEAD)
    values = (projected[:, 2] + bias_qv[1]).astype(jnp.bfloat16).reshape(seq_rows, heads_here, HEAD)
    scores = causal_scores(queries, key_heads, inv_root)
    row_peak = jnp.max(scores, axis=-1, keepdims=True)
    exp_terms = jnp.exp(scores - row_peak)
    exp_total = jnp.sum(exp_terms, axis=-1, keepdims=True)
    log_total = row_peak + jnp.log(exp_total)
    prob_low = (exp_terms / exp_total).astype(jnp.bfloat16)
    mixed_heads = (
        jnp.einsum("hqk,khd->qhd", prob_low, values, preferred_element_type=jnp.float32)
        .astype(jnp.bfloat16)
        .reshape(seq_rows, local_width)
    )
    attn_part = jnp.dot(mixed_heads, whole_out, preferred_element_type=jnp.float32)
    residual = inputs + lax.psum(attn_part.astype(jnp.bfloat16), "mp").astype(jnp.float32) + bias_out
    normed_two = layer_norm(residual, gain_two, shift_two).astype(jnp.bfloat16)
    preact = jnp.dot(normed_two, whole_fc1, preferred_element_type=jnp.float32) + bias_fc1
    activated = smooth_gate(preact).astype(jnp.bfloat16)
    ffn_part = jnp.dot(activated, whole_fc2, preferred_element_type=jnp.float32)
    out_tokens = (
        residual + lax.psum(ffn_part.astype(jnp.bfloat16), "mp").astype(jnp.float32) + bias_fc2
    ).astype(jnp.bfloat16)
    dp_index = lax.axis_index("dp")
    slot_ids = lax.iota(jnp.int32, counts.shape[0])
    own_count = jnp.sum(jnp.where(slot_ids == dp_index, counts, 0))
    weight_share = own_count.astype(jnp.float32) / jnp.sum(counts).astype(jnp.float32)
    live_rows = lax.iota(jnp.int32, seq_rows) < own_count
    grad_out = jnp.where(live_rows[:, None], cotangent.astype(jnp.float32), 0.0)
    grad_out_low = grad_out.astype(jnp.bfloat16)
    grad_fc2 = (
        jnp.einsum("sf,sd->fd", activated, grad_out_low, preferred_element_type=jnp.float32)
        * weight_share
    )
    grad_fc2_bias = jnp.sum(grad_out, axis=0) * weight_share
    delta_act = jnp.einsum("sd,fd->sf", grad_out_low, whole_fc2, preferred_element_type=jnp.float32)
    unused_gate, gate_back = jax.vjp(smooth_gate, preact)
    delta_pre = gate_back(delta_act)[0]
    grad_fc1_bias = jnp.sum(delta_pre, axis=0) * weight_share
    delta_pre_low = delta_pre.astype(jnp.bfloat16)
    grad_fc1 = (
        jnp.einsum("sd,sf->df", normed_two, delta_pre_low, preferred_element_type=jnp.float32)
        * weight_share
    )
    two_part = jnp.einsum("sf,df->sd", delta_pre_low, whole_fc1, preferred_element_type=jnp.float32)
    delta_two = lax.psum(two_part.astype(jnp.bfloat16), "mp").astype(jnp.float32)
    unused_two, second_back = jax.vjp(layer_norm, residual, gain_two, shift_two)
    resid_part, gain_two_part, shift_two_part = second_back(delta_two)
    delta_resid = resid_part + grad_out
    delta_resid_low = delta_resid.astype(jnp.bfloat16)
    out_bias_part = jnp.sum(delta_resid, axis=0)
    grad_out_proj = (
        jnp.einsum("sc,sd->cd", mixed_heads, delta_resid_low, preferred_element_type=jnp.float32)
        * weight_share
    )
    delta_mixed = jnp.einsum(
        "sd,cd->sc", delta_resid_low, whole_out, preferred_element_type=jnp.float32
    )
    delta_mixed_low = delta_mixed.astype(jnp.bfloat16).reshape(seq_rows, heads_here, HEAD)
    scores_again = causal_scores(queries, key_heads, inv_root)
    prob_full = jnp.exp(scores_again - log_total)
    delta_prob = jnp.einsum(
        "qhd,khd->hqk", delta_mixed_low, values, preferred_element_type=jnp.float32
    )
    delta_scores = prob_full * (
        delta_prob - jnp.sum(prob_full * delta_prob, axis=-1, keepdims=True)
    )
    delta_scores_low = delta_scores.astype(jnp.bfloat16)
    delta_q = (
        jnp.einsum("hqk,khd->qhd", delta_scores_low, key_heads, preferred_element_type=jnp.float32)
        * inv_root
    ).reshape(seq_rows, local_width)
    delta_k = (
        jnp.einsum("hqk,qhd->khd", delta_scores_low, queries, preferred_element_type=jnp.float32)
        * inv_root
    ).reshape(seq_rows, local_width)
    delta_v = jnp.einsum(
        "hqk,qhd->khd", prob_low, delta_mixed_low, preferred_element_type=jnp.float32
    ).reshape(seq_rows, local_width)
    grad_qv = jnp.stack([jnp.sum(delta_q, axis=0), jnp.sum(delta_v, axis=0)]) * weight_share
    delta_proj = jnp.stack([delta_q, delta_k, delta_v], axis=1).astype(jnp.bfloat16)
    grad_qkv = (
        jnp.einsum("sd,sce->dce", normed_one, delta_proj, preferred_element_type=jnp.float32)
        * weight_share
    )
    one_part = jnp.einsum("sce,dce->sd", delta_proj, whole_qkv, preferred_element_type=jnp.float32)
    delta_one = lax.psum(one_part.astype(jnp.bfloat16), "mp").astype(jnp.float32)
    unused_one, first_back = jax.vjp(layer_norm, inputs, gain_one, shift_one)
    input_part, gain_one_part, shift_one_part = first_back(delta_one)
    grad_tokens = input_part + delta_resid
    grad_vectors = (
        gain_one_part * weight_share,
        shift_one_part * weight_share,
        gain_two_part * weight_share,
        shift_two_part * weight_share,
        out_bias_part * weight_share,
        grad_fc2_bias,
        grad_fc1_bias,
    )
    stacked = jnp.concatenate(
        [vector.reshape(n_dp, -1) for vector in grad_vectors]
        + [grad_qv.reshape(2, n_dp, -1).transpose(1, 0, 2).reshape(n_dp, -1)],
        axis=1,
    )
    own = lax.psum_scatter(stacked, "dp", scatter_dimension=0, tiled=True)[0]
    pieces = []
    at = 0
    for vector in vectors:
        pieces.append(own[at : at + vector.shape[0]])
        at += vector.shape[0]

    def scatter(grad, axis):
        low = grad.astype(jnp.bfloat16)
        return lax.psum_scatter(low, "dp", scatter_dimension=axis, tiled=True).astype(jnp.float32)

    return (
        out_tokens,
        grad_tokens,
        scatter(grad_qkv, 0),
        scatter(grad_out_proj, 1),
        scatter(grad_fc1, 0),
        scatter(grad_fc2, 1),
        pieces[0],
        pieces[1],
        pieces[2],
        pieces[3],
        pieces[7].reshape(2, -1),
        pieces[4],
        pieces[6],
        pieces[5],
    )


def solution(mesh):
    placed = (
        P("dp", None),
        P("dp", None),
        P(),
        P("dp", None, "mp"),
        P("mp", "dp"),
        P("dp", "mp"),
        P("mp", "dp"),
        P("dp"),
        P("dp"),
        P("dp"),
        P("dp"),
        P(None, ("mp", "dp")),
        P("dp"),
        P(("mp", "dp")),
        P("dp"),
    )
    return jax.shard_map(
        shards,
        mesh=mesh,
        in_specs=placed,
        out_specs=(
            P("dp", None),
            P("dp", None),
            P("dp", None, "mp"),
            P("mp", "dp"),
            P("dp", "mp"),
            P("mp", "dp"),
            P("dp"),
            P("dp"),
            P("dp"),
            P("dp"),
            P(None, ("mp", "dp")),
            P("dp"),
            P(("mp", "dp")),
            P("dp"),
        ),
        check_vma=False,
    )
```

```python
import functools
import math

import jax
import jax.numpy as jnp
from jax import lax
from jax.experimental import pallas as pl
from jax.experimental.pallas import tpu as pltpu
from jax.sharding import PartitionSpec as P

HEAD = 128
QROWS = 256
BLOCKS = 8
MESH = pl.DeviceIdType.MESH


EPS = 1e-05
NEG = -1e30


def layer_norm(values, gain_vec, shift_vec):
    center = values - jnp.mean(values, axis=-1, keepdims=True)
    spread = jnp.mean(center * center, axis=-1, keepdims=True)
    return center * lax.rsqrt(spread + EPS) * gain_vec + shift_vec


def smooth_gate(values):
    return jax.nn.gelu(values, approximate=True)


def future_mask(start, width, rows):
    keys = lax.broadcasted_iota(jnp.int32, (width, rows), 0)
    return keys > start + lax.broadcasted_iota(jnp.int32, (width, rows), 1)

def attend_kernel(inv_root, q_ref, k_ref, v_ref, mixed_ref, lse_ref):
    seq = q_ref.shape[0]
    for start in range(0, seq, QROWS):
        width = start + QROWS
        scores = lax.dot_general(k_ref[:width], q_ref[start:width], (((1,), (1,)), ((), ())),
            preferred_element_type=jnp.float32) * inv_root
        scores = jnp.where(future_mask(start, width, QROWS), NEG, scores)
        peak = jnp.max(scores, axis=0, keepdims=True)
        terms = jnp.exp(scores - peak)
        total = jnp.sum(terms, axis=0, keepdims=True)
        lse_ref[0, :, start:width] = peak + jnp.log(total)
        prob = (terms / total).astype(jnp.bfloat16)
        mixed = lax.dot_general(v_ref[:width], prob, (((0,), (0,)), ((), ())), preferred_element_type=jnp.float32)
        mixed_ref[start:width] = mixed.T.astype(jnp.bfloat16)

def attend(qkv, heads):
    seq = qkv.shape[0]
    col = lambda c: pl.BlockSpec((seq, HEAD), lambda h, c=c: (0, c * heads + h))
    return pl.pallas_call(
        functools.partial(attend_kernel, 1.0 / math.sqrt(HEAD)),
        grid=(heads,), in_specs=[col(0), col(1), col(2)],
        out_specs=[pl.BlockSpec((seq, HEAD), lambda h: (0, h)), pl.BlockSpec((1, 1, seq), lambda h: (h, 0, 0))],
        out_shape=[jax.ShapeDtypeStruct((seq, heads * HEAD), jnp.bfloat16), jax.ShapeDtypeStruct((heads, 1, seq), jnp.float32)],
        name="attend")(qkv, qkv, qkv)

def attend_back_kernel(inv_root, heads, q_ref, k_ref, v_ref, g_ref, lse_ref, out_ref, sums_ref, dk_acc, dv_acc):
    seq = q_ref.shape[0]
    head = pl.program_id(0)
    dk_acc[...] = jnp.zeros_like(dk_acc)
    dv_acc[...] = jnp.zeros_like(dv_acc)
    cols = [pl.ds(pl.multiple_of((c * heads + head) * HEAD, HEAD), HEAD) for c in range(3)]
    dq_sum = jnp.zeros((1, HEAD), jnp.float32)
    for start in range(0, seq, QROWS):
        width = start + QROWS
        q = q_ref[start:width]
        g = g_ref[start:width]
        k = k_ref[:width]
        nt = (((1,), (1,)), ((), ()))
        scores = lax.dot_general(k, q, nt, preferred_element_type=jnp.float32) * inv_root
        scores = jnp.where(future_mask(start, width, QROWS), NEG, scores)
        prob = jnp.exp(scores - lse_ref[0, :, start:width])
        dprob = lax.dot_general(v_ref[:width], g, nt, preferred_element_type=jnp.float32)
        ds = (prob * (dprob - jnp.sum(prob * dprob, axis=0, keepdims=True))).astype(jnp.bfloat16)
        dv_acc[:width] += jnp.dot(prob.astype(jnp.bfloat16), g, preferred_element_type=jnp.float32)
        dk_acc[:width] += jnp.dot(ds, q, preferred_element_type=jnp.float32)
        dq = lax.dot_general(k, ds, (((0,), (0,)), ((), ())), preferred_element_type=jnp.float32).T * inv_root
        out_ref[start:width, cols[0]] = dq.astype(jnp.bfloat16)
        dq_sum += jnp.sum(dq, axis=0, keepdims=True)
    out_ref[:, cols[1]] = (dk_acc[...] * inv_root).astype(jnp.bfloat16)
    dv = dv_acc[...]
    out_ref[:, cols[2]] = dv.astype(jnp.bfloat16)
    sums_ref[0, 0:1] = dq_sum
    sums_ref[0, 1:2] = jnp.sum(dv, axis=0, keepdims=True)

def attend_back(qkv, grad, lse, heads):
    seq = qkv.shape[0]
    col = lambda c: pl.BlockSpec((seq, HEAD), lambda h, c=c: (0, c * heads + h))
    return pl.pallas_call(
        functools.partial(attend_back_kernel, 1.0 / math.sqrt(HEAD), heads),
        grid=(heads,), in_specs=[col(0), col(1), col(2), col(0), pl.BlockSpec((1, 1, seq), lambda h: (h, 0, 0))],
        out_specs=[pl.BlockSpec((seq, 3 * heads * HEAD), lambda h: (0, 0)), pl.BlockSpec((1, 2, HEAD), lambda h: (h, 0, 0))],
        out_shape=[jax.ShapeDtypeStruct((seq, 3 * heads * HEAD), jnp.bfloat16), jax.ShapeDtypeStruct((heads, 2, HEAD), jnp.float32)],
        scratch_shapes=[pltpu.VMEM((seq, HEAD), jnp.float32)] * 2, name="attend_back")(qkv, qkv, qkv, grad, lse)


def chain_kernel(n, blocks, x_ref, o_ref, held, s1, r1, s2, r2):
    me = lax.axis_index("mp")
    rows = x_ref.shape[0] // (2 * blocks)
    right = lax.rem(me + 1, n); left = lax.rem(me + n - 1, n)
    barrier = pltpu.get_barrier_semaphore()
    last = n - 1

    @pl.when(me > 0)
    def _():
        pl.semaphore_signal(barrier, inc=1, device_id={"mp": left}, device_id_type=MESH)

    @pl.when(me < last)
    def _():
        pl.semaphore_signal(barrier, inc=1, device_id={"mp": right}, device_id_type=MESH)

    pl.semaphore_wait(barrier, jnp.where(me > 0, 1, 0) + jnp.where(me < last, 1, 0))

    def sl(half, b):
        return pl.ds(pl.multiple_of((half * blocks + b) * rows, rows), rows)

    def reduce_copy(half, b, src, target):
        return pltpu.make_async_remote_copy(src_ref=src.at[sl(half, b)], dst_ref=held.at[sl(half, b)],
            send_sem=s1.at[half * blocks + b], recv_sem=r1.at[half * blocks + b], device_id={"mp": target}, device_id_type=MESH)
    def cast_copy(half, b, target):
        return pltpu.make_async_remote_copy(src_ref=o_ref.at[sl(half, b)], dst_ref=o_ref.at[sl(half, b)],
            send_sem=s2.at[half * blocks + b], recv_sem=r2.at[half * blocks + b], device_id={"mp": target}, device_id_type=MESH)

    def step(t, carry):
        for half, pos, fwd, back in ((0, me, right, left), (1, last - me, left, right)):
            b = t - pos
            live = jnp.logical_and(b >= 0, b < blocks)
            @pl.when(jnp.logical_and(live, pos == 0))
            def _():
                reduce_copy(half, b, x_ref, fwd).start()
            @pl.when(jnp.logical_and(live, pos > 0))
            def _():
                reduce_copy(half, b, x_ref, fwd).wait_recv()
                total = held[sl(half, b)].astype(jnp.float32) + x_ref[sl(half, b)].astype(jnp.float32)
                @pl.when(pos < last)
                def _():
                    held[sl(half, b)] = total.astype(jnp.bfloat16)
                    reduce_copy(half, b, held, fwd).start()
                @pl.when(pos == last)
                def _():
                    o_ref[sl(half, b)] = total.astype(jnp.bfloat16)
                    cast_copy(half, b, back).start()
        for half, pos, fwd, back in ((0, me, right, left), (1, last - me, left, right)):
            b = t - (2 * last - pos)
            live = jnp.logical_and(b >= 0, b < blocks)
            @pl.when(jnp.logical_and(live, pos < last))
            def _():
                cast_copy(half, b, back).wait_recv()
                @pl.when(pos > 0)
                def _():
                    cast_copy(half, b, back).start()
        return carry
    lax.fori_loop(0, blocks + 2 * last, step, 0)
    def drain(b, carry):
        for half, pos in ((0, me), (1, last - me)):
            @pl.when(pos == 0)
            def _(): reduce_copy(half, b, x_ref, right).wait_send()
            @pl.when(jnp.logical_and(pos > 0, pos < last))
            def _(): reduce_copy(half, b, held, right).wait_send()
            @pl.when(pos > 0)
            def _(): cast_copy(half, b, left).wait_send()
        return carry
    lax.fori_loop(0, blocks, drain, 0)

def all_reduce(x, n, blocks, cid):
    nb = 2 * blocks
    vm = pl.BlockSpec(memory_space=pltpu.VMEM)
    return pl.pallas_call(functools.partial(chain_kernel, n, blocks),
        out_shape=jax.ShapeDtypeStruct(x.shape, x.dtype), in_specs=[vm], out_specs=vm,
        scratch_shapes=[pltpu.VMEM(x.shape, x.dtype)] + [pltpu.SemaphoreType.DMA((nb,))] * 4,
        compiler_params=pltpu.CompilerParams(collective_id=cid, has_side_effects=True, vmem_limit_bytes=20 << 20))(x)


def shards(
    tokens,
    cotangent,
    counts,
    w_qkv,
    w_out,
    w_fc1,
    w_fc2,
    ln1_gain,
    ln1_bias,
    ln2_gain,
    ln2_bias,
    qv_bias,
    out_bias,
    fc1_bias,
    fc2_bias,
):
    whole_qkv = lax.all_gather(w_qkv.reshape(w_qkv.shape[0], -1), "dp", axis=0, tiled=True)
    whole_out = lax.all_gather(w_out, "dp", axis=1, tiled=True)
    whole_fc1 = lax.all_gather(w_fc1, "dp", axis=0, tiled=True)
    whole_fc2 = lax.all_gather(w_fc2, "dp", axis=1, tiled=True)
    vectors = (
        ln1_gain,
        ln1_bias,
        ln2_gain,
        ln2_bias,
        out_bias,
        fc2_bias,
        fc1_bias,
        qv_bias.reshape(-1),
    )
    packed = lax.all_gather(jnp.concatenate(vectors), "dp", axis=0).astype(jnp.float32)
    wide = []
    at = 0
    for vector in vectors:
        wide.append(packed[:, at : at + vector.shape[0]])
        at += vector.shape[0]
    gain_one, shift_one, gain_two, shift_two, bias_out, bias_fc2, bias_fc1 = (
        part.reshape(-1) for part in wide[:7]
    )
    n_dp = packed.shape[0]
    n_mp = lax.axis_size("mp")
    bias_qv = wide[7].reshape(n_dp, 2, -1).transpose(1, 0, 2).reshape(2, -1)
    seq_rows = tokens.shape[0]
    local_width = w_qkv.shape[2]
    heads_here = local_width // HEAD
    inputs = tokens.astype(jnp.float32)
    normed_one = layer_norm(inputs, gain_one, shift_one).astype(jnp.bfloat16)
    bias_all = jnp.concatenate([bias_qv[0], jnp.zeros_like(bias_qv[0]), bias_qv[1]])
    qkv = (
        jnp.dot(normed_one, whole_qkv, preferred_element_type=jnp.float32) + bias_all
    ).astype(jnp.bfloat16)
    mixed_heads, log_total = attend(qkv, heads_here)
    attn_part = jnp.dot(mixed_heads, whole_out, preferred_element_type=jnp.float32)
    residual = inputs + all_reduce(attn_part.astype(jnp.bfloat16), n_mp, BLOCKS, 0).astype(jnp.float32) + bias_out
    normed_two = layer_norm(residual, gain_two, shift_two).astype(jnp.bfloat16)
    preact = jnp.dot(normed_two, whole_fc1, preferred_element_type=jnp.float32) + bias_fc1
    activated = smooth_gate(preact).astype(jnp.bfloat16)
    ffn_part = jnp.dot(activated, whole_fc2, preferred_element_type=jnp.float32)
    out_tokens = (
        residual + lax.psum(ffn_part.astype(jnp.bfloat16), "mp").astype(jnp.float32) + bias_fc2
    ).astype(jnp.bfloat16)
    dp_index = lax.axis_index("dp")
    slot_ids = lax.iota(jnp.int32, counts.shape[0])
    own_count = jnp.sum(jnp.where(slot_ids == dp_index, counts, 0))
    weight_share = own_count.astype(jnp.float32) / jnp.sum(counts).astype(jnp.float32)
    live_rows = lax.iota(jnp.int32, seq_rows) < own_count
    grad_out = jnp.where(live_rows[:, None], cotangent.astype(jnp.float32), 0.0)
    grad_out_low = grad_out.astype(jnp.bfloat16)
    grad_fc2 = (
        jnp.einsum("sf,sd->fd", activated, grad_out_low, preferred_element_type=jnp.float32)
        * weight_share
    )
    grad_fc2_bias = jnp.sum(grad_out, axis=0) * weight_share
    delta_act = jnp.einsum("sd,fd->sf", grad_out_low, whole_fc2, preferred_element_type=jnp.float32)
    unused_gate, gate_back = jax.vjp(smooth_gate, preact)
    delta_pre = gate_back(delta_act)[0]
    grad_fc1_bias = jnp.sum(delta_pre, axis=0) * weight_share
    delta_pre_low = delta_pre.astype(jnp.bfloat16)
    grad_fc1 = (
        jnp.einsum("sd,sf->df", normed_two, delta_pre_low, preferred_element_type=jnp.float32)
        * weight_share
    )
    two_part = jnp.einsum("sf,df->sd", delta_pre_low, whole_fc1, preferred_element_type=jnp.float32)
    delta_two = all_reduce(two_part.astype(jnp.bfloat16), n_mp, BLOCKS, 0).astype(jnp.float32)
    unused_two, second_back = jax.vjp(layer_norm, residual, gain_two, shift_two)
    resid_part, gain_two_part, shift_two_part = second_back(delta_two)
    delta_resid = resid_part + grad_out
    delta_resid_low = delta_resid.astype(jnp.bfloat16)
    out_bias_part = jnp.sum(delta_resid, axis=0)
    grad_out_proj = (
        jnp.einsum("sc,sd->cd", mixed_heads, delta_resid_low, preferred_element_type=jnp.float32)
        * weight_share
    )
    delta_mixed = jnp.einsum(
        "sd,cd->sc", delta_resid_low, whole_out, preferred_element_type=jnp.float32
    )
    delta_mixed_low = delta_mixed.astype(jnp.bfloat16)
    delta_proj, qv_sums = attend_back(qkv, delta_mixed_low, log_total, heads_here)
    grad_qv = qv_sums.transpose(1, 0, 2).reshape(2, -1) * weight_share
    grad_qkv = (
        jnp.einsum("sd,se->de", normed_one, delta_proj, preferred_element_type=jnp.float32)
        * weight_share
    )
    one_part = jnp.einsum("se,de->sd", delta_proj, whole_qkv, preferred_element_type=jnp.float32)
    delta_one = all_reduce(one_part.astype(jnp.bfloat16), n_mp, BLOCKS, 0).astype(jnp.float32)
    unused_one, first_back = jax.vjp(layer_norm, inputs, gain_one, shift_one)
    input_part, gain_one_part, shift_one_part = first_back(delta_one)
    grad_tokens = input_part + delta_resid
    grad_vectors = (
        gain_one_part * weight_share,
        shift_one_part * weight_share,
        gain_two_part * weight_share,
        shift_two_part * weight_share,
        out_bias_part * weight_share,
        grad_fc2_bias,
        grad_fc1_bias,
    )
    stacked = jnp.concatenate(
        [vector.reshape(n_dp, -1) for vector in grad_vectors]
        + [grad_qv.reshape(2, n_dp, -1).transpose(1, 0, 2).reshape(n_dp, -1)],
        axis=1,
    )
    own = lax.psum_scatter(stacked, "dp", scatter_dimension=0, tiled=True)[0]
    pieces = []
    at = 0
    for vector in vectors:
        pieces.append(own[at : at + vector.shape[0]])
        at += vector.shape[0]

    def scatter(grad, axis):
        low = grad.astype(jnp.bfloat16)
        return lax.psum_scatter(low, "dp", scatter_dimension=axis, tiled=True).astype(jnp.float32)

    return (
        out_tokens,
        grad_tokens,
        scatter(grad_qkv, 0).reshape(w_qkv.shape),
        scatter(grad_out_proj, 1),
        scatter(grad_fc1, 0),
        scatter(grad_fc2, 1),
        pieces[0],
        pieces[1],
        pieces[2],
        pieces[3],
        pieces[7].reshape(2, -1),
        pieces[4],
        pieces[6],
        pieces[5],
    )


def solution(mesh):
    placed = (
        P("dp", None),
        P("dp", None),
        P(),
        P("dp", None, "mp"),
        P("mp", "dp"),
        P("dp", "mp"),
        P("mp", "dp"),
        P("dp"),
        P("dp"),
        P("dp"),
        P("dp"),
        P(None, ("mp", "dp")),
        P("dp"),
        P(("mp", "dp")),
        P("dp"),
    )
    return jax.shard_map(
        shards,
        mesh=mesh,
        in_specs=placed,
        out_specs=(
            P("dp", None),
            P("dp", None),
            P("dp", None, "mp"),
            P("mp", "dp"),
            P("dp", "mp"),
            P("mp", "dp"),
            P("dp"),
            P("dp"),
            P("dp"),
            P("dp"),
            P(None, ("mp", "dp")),
            P("dp"),
            P(("mp", "dp")),
            P("dp"),
        ),
        check_vma=False,
    )
```

```python
import functools
import math

import jax
import jax.numpy as jnp
from jax import lax
from jax.experimental import pallas as pl
from jax.experimental.pallas import tpu as pltpu
from jax.sharding import PartitionSpec as P

HEAD = 128
QROWS = 256
BLOCKS = 8
SUB = 2
VMEM_ALL = 67043328
MESH = pl.DeviceIdType.MESH


EPS = 1e-05
NEG = -1e30


def layer_norm(values, gain_vec, shift_vec):
    center = values - jnp.mean(values, axis=-1, keepdims=True)
    spread = jnp.mean(center * center, axis=-1, keepdims=True)
    return center * lax.rsqrt(spread + EPS) * gain_vec + shift_vec


def future_mask(start, width, rows):
    keys = lax.broadcasted_iota(jnp.int32, (width, rows), 0)
    return keys > start + lax.broadcasted_iota(jnp.int32, (width, rows), 1)

def attend_kernel(inv_root, q_ref, k_ref, v_ref, mixed_ref, lse_ref):
    seq = q_ref.shape[0]
    for start in range(0, seq, QROWS):
        width = start + QROWS
        scores = lax.dot_general(k_ref[:width], q_ref[start:width], (((1,), (1,)), ((), ())),
            preferred_element_type=jnp.float32) * inv_root
        scores = jnp.where(future_mask(start, width, QROWS), NEG, scores)
        peak = jnp.max(scores, axis=0, keepdims=True)
        terms = jnp.exp(scores - peak)
        total = jnp.sum(terms, axis=0, keepdims=True)
        lse_ref[0, :, start:width] = peak + jnp.log(total)
        prob = (terms / total).astype(jnp.bfloat16)
        mixed = lax.dot_general(v_ref[:width], prob, (((0,), (0,)), ((), ())), preferred_element_type=jnp.float32)
        mixed_ref[start:width] = mixed.T.astype(jnp.bfloat16)

def attend(qkv, heads):
    seq = qkv.shape[0]
    col = lambda c: pl.BlockSpec((seq, HEAD), lambda h, c=c: (0, c * heads + h))
    return pl.pallas_call(
        functools.partial(attend_kernel, 1.0 / math.sqrt(HEAD)),
        grid=(heads,), in_specs=[col(0), col(1), col(2)],
        out_specs=[pl.BlockSpec((seq, HEAD), lambda h: (0, h)), pl.BlockSpec((1, 1, seq), lambda h: (h, 0, 0))],
        out_shape=[jax.ShapeDtypeStruct((seq, heads * HEAD), jnp.bfloat16), jax.ShapeDtypeStruct((heads, 1, seq), jnp.float32)],
        name="attend")(qkv, qkv, qkv)

def attend_back_kernel(inv_root, heads, q_ref, k_ref, v_ref, g_ref, lse_ref, out_ref, sums_ref, dk_acc, dv_acc):
    seq = q_ref.shape[0]
    head = pl.program_id(0)
    dk_acc[...] = jnp.zeros_like(dk_acc)
    dv_acc[...] = jnp.zeros_like(dv_acc)
    cols = [pl.ds(pl.multiple_of((c * heads + head) * HEAD, HEAD), HEAD) for c in range(3)]
    dq_sum = jnp.zeros((1, HEAD), jnp.float32)
    for start in range(0, seq, QROWS):
        width = start + QROWS
        q = q_ref[start:width]
        g = g_ref[start:width]
        k = k_ref[:width]
        nt = (((1,), (1,)), ((), ()))
        scores = lax.dot_general(k, q, nt, preferred_element_type=jnp.float32) * inv_root
        scores = jnp.where(future_mask(start, width, QROWS), NEG, scores)
        prob = jnp.exp(scores - lse_ref[0, :, start:width])
        dprob = lax.dot_general(v_ref[:width], g, nt, preferred_element_type=jnp.float32)
        ds = (prob * (dprob - jnp.sum(prob * dprob, axis=0, keepdims=True))).astype(jnp.bfloat16)
        dv_acc[:width] += jnp.dot(prob.astype(jnp.bfloat16), g, preferred_element_type=jnp.float32)
        dk_acc[:width] += jnp.dot(ds, q, preferred_element_type=jnp.float32)
        dq = lax.dot_general(k, ds, (((0,), (0,)), ((), ())), preferred_element_type=jnp.float32).T * inv_root
        out_ref[start:width, cols[0]] = dq.astype(jnp.bfloat16)
        dq_sum += jnp.sum(dq, axis=0, keepdims=True)
    out_ref[:, cols[1]] = (dk_acc[...] * inv_root).astype(jnp.bfloat16)
    dv = dv_acc[...]
    out_ref[:, cols[2]] = dv.astype(jnp.bfloat16)
    sums_ref[0, 0:1] = dq_sum
    sums_ref[0, 1:2] = jnp.sum(dv, axis=0, keepdims=True)

def attend_back(qkv, grad, lse, heads):
    seq = qkv.shape[0]
    col = lambda c: pl.BlockSpec((seq, HEAD), lambda h, c=c: (0, c * heads + h))
    return pl.pallas_call(
        functools.partial(attend_back_kernel, 1.0 / math.sqrt(HEAD), heads),
        grid=(heads,), in_specs=[col(0), col(1), col(2), col(0), pl.BlockSpec((1, 1, seq), lambda h: (h, 0, 0))],
        out_specs=[pl.BlockSpec((seq, 3 * heads * HEAD), lambda h: (0, 0)), pl.BlockSpec((1, 2, HEAD), lambda h: (h, 0, 0))],
        out_shape=[jax.ShapeDtypeStruct((seq, 3 * heads * HEAD), jnp.bfloat16), jax.ShapeDtypeStruct((heads, 2, HEAD), jnp.float32)],
        scratch_shapes=[pltpu.VMEM((seq, HEAD), jnp.float32)] * 2, name="attend_back")(qkv, qkv, qkv, grad, lse)


NN = (((1,), (0,)), ((), ()))
NT = (((1,), (1,)), ((), ()))
GELU_A = math.sqrt(2.0 / math.pi)
GELU_B = 0.044715


def mat(left, right, dims):
    return lax.dot_general(left, right, dims, preferred_element_type=jnp.float32)


class Chain:
    def __init__(self, n, rows, part, held, total, sems):
        self.n, self.part, self.held, self.total = n, part, held, total
        self.s1, self.r1, self.s2, self.r2 = sems
        self.rows = rows // (2 * BLOCKS)
        self.me = lax.axis_index("mp")
        self.last = n - 1
        self.right = lax.rem(self.me + 1, n)
        self.left = lax.rem(self.me + n - 1, n)
        self.sides = (
            (0, self.me, self.right, self.left),
            (1, self.last - self.me, self.left, self.right),
        )
        self.steps = BLOCKS + 2 * self.last

    def start_row(self, half, b):
        return pl.multiple_of(
            ((b // SUB) * 2 * SUB + half * SUB + b % SUB) * self.rows, self.rows
        )

    def cut(self, half, b):
        return pl.ds(self.start_row(half, b), self.rows)

    def forward(self, half, b, src, target):
        return pltpu.make_async_remote_copy(
            src_ref=src.at[self.cut(half, b)],
            dst_ref=self.held.at[self.cut(half, b)],
            send_sem=self.s1.at[half * BLOCKS + b],
            recv_sem=self.r1.at[half * BLOCKS + b],
            device_id={"mp": target},
            device_id_type=MESH,
        )

    def back(self, half, b, target):
        return pltpu.make_async_remote_copy(
            src_ref=self.total.at[self.cut(half, b)],
            dst_ref=self.total.at[self.cut(half, b)],
            send_sem=self.s2.at[half * BLOCKS + b],
            recv_sem=self.r2.at[half * BLOCKS + b],
            device_id={"mp": target},
            device_id_type=MESH,
        )

    def step(self, t, arrived=None):
        for half, pos, ahead, behind in self.sides:
            b = t - pos
            live = jnp.logical_and(b >= 0, b < BLOCKS)

            @pl.when(jnp.logical_and(live, pos == 0))
            def _():
                self.forward(half, b, self.part, ahead).start()

            @pl.when(jnp.logical_and(live, pos > 0))
            def _():
                self.forward(half, b, self.part, ahead).wait_recv()
                cut = self.cut(half, b)
                both = self.held[cut].astype(jnp.float32) + self.part[cut].astype(jnp.float32)

                @pl.when(pos < self.last)
                def _():
                    self.held[cut] = both.astype(jnp.bfloat16)
                    self.forward(half, b, self.held, ahead).start()

                @pl.when(pos == self.last)
                def _():
                    self.total[cut] = both.astype(jnp.bfloat16)
                    self.back(half, b, behind).start()
                    if arrived is not None:
                        arrived(half, b, cut)

        for half, pos, ahead, behind in self.sides:
            b = t - (2 * self.last - pos)
            live = jnp.logical_and(b >= 0, b < BLOCKS)

            @pl.when(jnp.logical_and(live, pos < self.last))
            def _():
                self.back(half, b, behind).wait_recv()

                @pl.when(pos > 0)
                def _():
                    self.back(half, b, behind).start()

                if arrived is not None:
                    arrived(half, b, self.cut(half, b))

    def drain(self):
        def one(b, carry):
            for half, pos, ahead, behind in self.sides:

                @pl.when(pos == 0)
                def _():
                    self.forward(half, b, self.part, ahead).wait_send()

                @pl.when(jnp.logical_and(pos > 0, pos < self.last))
                def _():
                    self.forward(half, b, self.held, ahead).wait_send()

                @pl.when(pos > 0)
                def _():
                    self.back(half, b, behind).wait_send()

            return carry

        lax.fori_loop(0, BLOCKS, one, 0)


def chain_sems():
    return [pltpu.SemaphoreType.DMA((2 * BLOCKS,))] * 4


def greet(n):
    me = lax.axis_index("mp")
    barrier = pltpu.get_barrier_semaphore()

    @pl.when(me > 0)
    def _():
        pl.semaphore_signal(
            barrier, inc=1, device_id={"mp": lax.rem(me + n - 1, n)}, device_id_type=MESH
        )

    @pl.when(me < n - 1)
    def _():
        pl.semaphore_signal(barrier, inc=1, device_id={"mp": lax.rem(me + 1, n)}, device_id_type=MESH)

    pl.semaphore_wait(barrier, jnp.where(me > 0, 1, 0) + jnp.where(me < n - 1, 1, 0))


def moments(wide):
    center = wide - jnp.mean(wide, axis=-1, keepdims=True)
    scale = lax.rsqrt(jnp.mean(center * center, axis=-1, keepdims=True) + EPS)
    return center * scale, scale


def ffn_kernel(
    n, tok_hbm, att_hbm, g_hbm, w1_hbm, w2_hbm, vec_ref, b1_ref, share_ref,
    act_hbm, low_hbm, g1_hbm, g2_hbm, sums_ref, b1sum_ref,
    tok, att, g, w1, w2, act, dpre, nrm, part, held, total, stage, flip,
    in_sem, w_sem, out_sem, stage_sem, s1, r1, s2, r2,
):
    rows, d = tok.shape
    f = w1.shape[1]
    group = 2 * SUB * rows // (2 * BLOCKS)
    groups = rows // group
    tile = 512
    chain = Chain(n, rows, part, held, total, (s1, r1, s2, r2))
    small = chain.rows

    def load(src, dst, which, c):
        cut = pl.ds(pl.multiple_of(c * group, group), group)
        return pltpu.make_async_copy(src.at[cut], dst.at[cut], in_sem.at[which * groups + c])

    def load_group(c):
        load(tok_hbm, tok, 0, c).start()
        load(att_hbm, att, 1, c).start()
        load(g_hbm, g, 2, c).start()

    load_group(0)
    first_weight = pltpu.make_async_copy(w1_hbm, w1, w_sem.at[0])
    second_weight = pltpu.make_async_copy(w2_hbm, w2, w_sem.at[1])
    first_weight.start()
    second_weight.start()
    for c in range(1, groups):
        load_group(c)
    greet(n)
    sums_ref[...] = jnp.zeros_like(sums_ref)
    b1sum_ref[...] = jnp.zeros_like(b1sum_ref)
    gain = vec_ref[0:1]
    shift = vec_ref[1:2]
    out_bias = vec_ref[2:3]

    def act_out(c):
        cut = pl.ds(pl.multiple_of(c * group, group), group)
        return pltpu.make_async_copy(act.at[cut], act_hbm.at[cut], out_sem.at[c])

    def low_out(half, b):
        cut = chain.cut(half, b)
        return pltpu.make_async_copy(att.at[cut], low_hbm.at[cut], out_sem.at[groups + half * BLOCKS + b])

    def compute(c):
        load(tok_hbm, tok, 0, c).wait()
        load(att_hbm, att, 1, c).wait()

        def norm(i, carry):
            cut = pl.ds(pl.multiple_of(c * group + i * small, small), small)
            wide = tok[cut].astype(jnp.float32) + att[cut].astype(jnp.float32) + out_bias
            normal, _ = moments(wide)
            nrm[cut] = (normal * gain + shift).astype(jnp.bfloat16)
            return carry

        lax.fori_loop(0, group // small, norm, 0)
        load(g_hbm, g, 2, c).wait()

    def hidden(c):
        cut = pl.ds(pl.multiple_of(c * group, group), group)

        def one(j, carry):
            cols = pl.ds(pl.multiple_of(j * tile, tile), tile)
            pre = mat(nrm[cut], w1[:, cols], NN) + b1_ref[:, cols]
            square = pre * pre
            bend = jnp.tanh(GELU_A * (pre + GELU_B * (square * pre)))
            half_gate = 0.5 * (1.0 + bend)
            act[cut, cols] = (pre * half_gate).astype(jnp.bfloat16)
            slope = half_gate + 0.5 * pre * (1.0 - bend * bend) * (
                GELU_A * (1.0 + 3.0 * GELU_B * square)
            )
            delta = mat(g[cut], w2[cols, :], NT) * slope
            b1sum_ref[:, cols] += jnp.sum(delta, axis=0, keepdims=True)
            dpre[cut, cols] = delta.astype(jnp.bfloat16)
            return carry

        lax.fori_loop(0, f // tile, one, 0)
        act_out(c).start()

        def two(j, carry):
            cols = pl.ds(pl.multiple_of(j * tile, tile), tile)
            part[cut, cols] = mat(dpre[cut], w1[cols, :], NT).astype(jnp.bfloat16)
            return carry

        lax.fori_loop(0, d // tile, two, 0)

    def arrived(half, b, cut):
        wide = tok[cut].astype(jnp.float32) + att[cut].astype(jnp.float32) + out_bias
        normal, scale = moments(wide)
        delta = total[cut].astype(jnp.float32)
        dn = delta * gain
        inner = dn - jnp.mean(dn, axis=-1, keepdims=True)
        inner = inner - normal * jnp.mean(dn * normal, axis=-1, keepdims=True)
        whole = g[cut].astype(jnp.float32) + scale * inner
        att[cut] = whole.astype(jnp.bfloat16)
        low_out(half, b).start()
        sums_ref[0:1] += jnp.sum(delta * normal, axis=0, keepdims=True)
        sums_ref[1:2] += jnp.sum(delta, axis=0, keepdims=True)
        sums_ref[2:3] += jnp.sum(whole, axis=0, keepdims=True)

    def group_step(c, carry):
        compute(c)

        @pl.when(c == 0)
        def _():
            first_weight.wait()
            second_weight.wait()

        hidden(c)
        for k in range(SUB):
            chain.step(SUB * c + k, arrived)
        return carry

    lax.fori_loop(0, groups, group_step, 0)

    share = share_ref[0, 0]
    side = 256
    tiles_one, tiles_two = d // side, f // side
    count = tiles_one + tiles_two

    def stage_out(i):
        slot = i % 2

        def one():
            return pltpu.make_async_copy(
                stage.at[slot, :, pl.ds(0, f)],
                g1_hbm.at[pl.ds(pl.multiple_of(i * side, side), side)],
                stage_sem.at[slot],
            )

        def two():
            return pltpu.make_async_copy(
                stage.at[slot, :, pl.ds(0, d)],
                g2_hbm.at[pl.ds(pl.multiple_of((i - tiles_one) * side, side), side)],
                stage_sem.at[slot],
            )

        return one, two

    def wait_stage(i):
        one, two = stage_out(i)

        @pl.when(i < tiles_one)
        def _():
            one().wait()

        @pl.when(i >= tiles_one)
        def _():
            two().wait()

    def grads(i):
        slot = i % 2

        @pl.when(i >= 2)
        def _():
            wait_stage(i - 2)

        one, two = stage_out(i)

        def run(left, right, width, at):
            flip[...] = left[:, pl.ds(pl.multiple_of(at * side, side), side)].T

            def tile_of(j, carry):
                cols = pl.ds(pl.multiple_of(j * tile, tile), tile)
                stage[slot, :, cols] = (mat(flip[...], right[:, cols], NN) * share).astype(
                    jnp.bfloat16
                )
                return carry

            lax.fori_loop(0, width // tile, tile_of, 0)

        @pl.when(i < tiles_one)
        def _():
            run(nrm, dpre, f, i)
            one().start()

        @pl.when(i >= tiles_one)
        def _():
            run(act, g, d, i - tiles_one)
            two().start()

    extra = 2 * (n - 1)
    each = -(-count // extra)

    def tail(t, carry):
        for k in range(each):
            i = t * each + k

            @pl.when(i < count)
            def _():
                grads(i)

        chain.step(BLOCKS + t, arrived)
        return carry

    lax.fori_loop(0, extra, tail, 0)
    chain.drain()
    for i in (count - 2, count - 1):
        wait_stage(i)

    def settle(b, carry):
        for half in (0, 1):
            low_out(half, b).wait()
        return carry

    lax.fori_loop(0, BLOCKS, settle, 0)
    for c in range(groups):
        act_out(c).wait()


def ffn(tokens, summed, grad_low, whole_fc1, whole_fc2, vectors, bias_fc1, share, n, cid):
    rows, d = tokens.shape
    f = whole_fc1.shape[1]
    groups = BLOCKS // SUB
    anywhere = pl.BlockSpec(memory_space=pl.ANY)
    vm = pl.BlockSpec(memory_space=pltpu.VMEM)
    low = lambda *shape: pltpu.VMEM(shape, jnp.bfloat16)
    return pl.pallas_call(
        functools.partial(ffn_kernel, n),
        out_shape=[
            jax.ShapeDtypeStruct((rows, f), jnp.bfloat16),
            jax.ShapeDtypeStruct((rows, d), jnp.bfloat16),
            jax.ShapeDtypeStruct((d, f), jnp.bfloat16),
            jax.ShapeDtypeStruct((f, d), jnp.bfloat16),
            jax.ShapeDtypeStruct((3, d), jnp.float32),
            jax.ShapeDtypeStruct((1, f), jnp.float32),
        ],
        in_specs=[anywhere] * 5 + [vm, vm, pl.BlockSpec(memory_space=pltpu.SMEM)],
        out_specs=[anywhere] * 4 + [vm, vm],
        scratch_shapes=[
            low(rows, d), low(rows, d), low(rows, d), low(d, f), low(f, d),
            low(rows, f), low(rows, f), low(rows, d), low(rows, d), low(rows, d), low(rows, d),
            low(2, 256, max(d, f)), low(256, rows),
            pltpu.SemaphoreType.DMA((3 * groups,)),
            pltpu.SemaphoreType.DMA((2,)),
            pltpu.SemaphoreType.DMA((groups + 2 * BLOCKS,)),
            pltpu.SemaphoreType.DMA((2,)),
        ] + chain_sems(),
        compiler_params=pltpu.CompilerParams(
            collective_id=cid, has_side_effects=True, vmem_limit_bytes=VMEM_ALL
        ),
        name="ffn",
    )(tokens, summed, grad_low, whole_fc1, whole_fc2, vectors, bias_fc1, share)


def mix_kernel(n, mixed_ref, w_ref, total, part, held, s1, r1, s2, r2):
    rows = mixed_ref.shape[0]
    group = SUB * rows // BLOCKS
    chain = Chain(n, rows, part, held, total, (s1, r1, s2, r2))
    greet(n)

    def group_step(c, carry):
        cut = pl.ds(pl.multiple_of(c * group, group), group)
        part[cut] = mat(mixed_ref[cut], w_ref[...], NN).astype(jnp.bfloat16)
        for k in range(SUB):
            chain.step(SUB * c + k)
        return carry

    lax.fori_loop(0, rows // group, group_step, 0)
    lax.fori_loop(BLOCKS, chain.steps, lambda t, carry: (chain.step(t), carry)[1], 0)
    chain.drain()


def mix(mixed, whole_out, n, cid):
    rows, d = mixed.shape[0], whole_out.shape[1]
    vm = pl.BlockSpec(memory_space=pltpu.VMEM)
    return pl.pallas_call(
        functools.partial(mix_kernel, n),
        out_shape=jax.ShapeDtypeStruct((rows, d), jnp.bfloat16),
        in_specs=[vm, vm],
        out_specs=vm,
        scratch_shapes=[pltpu.VMEM((rows, d), jnp.bfloat16)] * 2 + chain_sems(),
        compiler_params=pltpu.CompilerParams(
            collective_id=cid, has_side_effects=True, vmem_limit_bytes=28 << 20
        ),
        name="mix",
    )(mixed, whole_out)


def close_kernel(
    n, dproj_hbm, wq_hbm, tok_hbm, low_hbm, att_hbm, act_hbm, w2_hbm, vec_ref,
    out_hbm, gtok_hbm, sums_ref,
    dproj, wq, tok, low, att, act, w2, part_one, held_one, total_one, part_two, held_two, total_two,
    in_sem, out_sem, s1, r1, s2, r2, s3, r3, s4, r4,
):
    rows, d = tok.shape
    f = w2.shape[0]
    group = SUB * rows // BLOCKS
    tile = 512
    one = Chain(n, rows, part_one, held_one, total_one, (s1, r1, s2, r2))
    two = Chain(n, rows, part_two, held_two, total_two, (s3, r3, s4, r4))
    pairs = (
        (dproj_hbm, dproj), (wq_hbm, wq), (act_hbm, act), (w2_hbm, w2),
        (tok_hbm, tok), (att_hbm, att), (low_hbm, low),
    )
    loads = [pltpu.make_async_copy(a, b, in_sem.at[i]) for i, (a, b) in enumerate(pairs)]
    for copy in loads:
        copy.start()
    greet(n)
    sums_ref[...] = jnp.zeros_like(sums_ref)
    gain = vec_ref[0:1]
    me = lax.axis_index("mp")
    head_flag = jnp.where(me == 0, 1.0, 0.0)
    tail_flag = jnp.where(me == n - 1, 1.0, 0.0)

    def one_out(half, b):
        cut = one.cut(half, b)
        return pltpu.make_async_copy(low.at[cut], gtok_hbm.at[cut], out_sem.at[half * BLOCKS + b])

    def two_out(half, b):
        cut = two.cut(half, b)
        return pltpu.make_async_copy(
            total_two.at[cut], out_hbm.at[cut], out_sem.at[(2 + half) * BLOCKS + b]
        )

    def arrived_one(half, b, cut):
        normal, scale = moments(tok[cut].astype(jnp.float32))
        delta = total_one[cut].astype(jnp.float32)
        dn = delta * gain
        inner = dn - jnp.mean(dn, axis=-1, keepdims=True)
        inner = inner - normal * jnp.mean(dn * normal, axis=-1, keepdims=True)
        low[cut] = (low[cut].astype(jnp.float32) + scale * inner).astype(jnp.bfloat16)
        one_out(half, b).start()
        sums_ref[0:1] += jnp.sum(delta * normal, axis=0, keepdims=True)
        sums_ref[1:2] += jnp.sum(delta, axis=0, keepdims=True)

    def arrived_two(half, b, cut):
        two_out(half, b).start()

    def group_step(c, carry):
        cut = pl.ds(pl.multiple_of(c * group, group), group)

        @pl.when(c == 0)
        def _():
            loads[0].wait()
            loads[1].wait()

        def first(j, carry):
            cols = pl.ds(pl.multiple_of(j * tile, tile), tile)
            part_one[cut, cols] = mat(dproj[cut], wq[cols, :], NT).astype(jnp.bfloat16)
            return carry

        lax.fori_loop(0, d // tile, first, 0)

        @pl.when(c == 0)
        def _():
            for copy in loads[2:]:
                copy.wait()

        one.step(SUB * c, arrived_one)
        half_rows = group // 2

        def second(j, carry):
            cols = pl.ds(pl.multiple_of(j * tile, tile), tile)
            for half, flag in ((0, head_flag), (1, tail_flag)):
                own = pl.ds(pl.multiple_of(c * group + half * half_rows, half_rows), half_rows)
                wide = tok[own, cols].astype(jnp.float32) + att[own, cols].astype(jnp.float32)
                part = mat(act[own], w2[:, cols], NN) + flag * (wide + vec_ref[1:2, cols])
                part_two[own, cols] = part.astype(jnp.bfloat16)
            return carry

        lax.fori_loop(0, d // tile, second, 0)
        for k in range(1, SUB):
            one.step(SUB * c + k, arrived_one)
        return carry

    lax.fori_loop(0, rows // group, group_step, 0)

    def later(t, carry):
        one.step(t, arrived_one)
        two.step(t - BLOCKS, arrived_two)
        return carry

    lax.fori_loop(BLOCKS, one.steps + BLOCKS, later, 0)
    one.drain()
    two.drain()

    def settle(b, carry):
        for half in (0, 1):
            one_out(half, b).wait()
            two_out(half, b).wait()
        return carry

    lax.fori_loop(0, BLOCKS, settle, 0)


def close(dproj, whole_qkv, tokens, low, summed, act, whole_fc2, vectors, n, cid):
    rows, d = tokens.shape
    anywhere = pl.BlockSpec(memory_space=pl.ANY)
    vm = pl.BlockSpec(memory_space=pltpu.VMEM)
    held = [pltpu.VMEM((rows, d), jnp.bfloat16)]
    like = lambda x: pltpu.VMEM(x.shape, jnp.bfloat16)
    return pl.pallas_call(
        functools.partial(close_kernel, n),
        out_shape=[
            jax.ShapeDtypeStruct((rows, d), jnp.bfloat16),
            jax.ShapeDtypeStruct((rows, d), jnp.bfloat16),
            jax.ShapeDtypeStruct((2, d), jnp.float32),
        ],
        in_specs=[anywhere] * 7 + [vm],
        out_specs=[anywhere] * 2 + [vm],
        scratch_shapes=[like(dproj), like(whole_qkv)] + held * 3 + [like(act), like(whole_fc2)]
        + held * 6
        + [pltpu.SemaphoreType.DMA((7,)), pltpu.SemaphoreType.DMA((4 * BLOCKS,))]
        + chain_sems() + chain_sems(),
        compiler_params=pltpu.CompilerParams(
            collective_id=cid, has_side_effects=True, vmem_limit_bytes=VMEM_ALL
        ),
        name="close",
    )(dproj, whole_qkv, tokens, low, summed, act, whole_fc2, vectors)


def shards(
    tokens,
    cotangent,
    counts,
    w_qkv,
    w_out,
    w_fc1,
    w_fc2,
    ln1_gain,
    ln1_bias,
    ln2_gain,
    ln2_bias,
    qv_bias,
    out_bias,
    fc1_bias,
    fc2_bias,
):
    whole_qkv = lax.all_gather(w_qkv.reshape(w_qkv.shape[0], -1), "dp", axis=0, tiled=True)
    whole_out = lax.all_gather(w_out, "dp", axis=1, tiled=True)
    whole_fc1 = lax.all_gather(w_fc1, "dp", axis=0, tiled=True)
    whole_fc2 = lax.all_gather(w_fc2, "dp", axis=1, tiled=True)
    vectors = (
        ln1_gain,
        ln1_bias,
        ln2_gain,
        ln2_bias,
        out_bias,
        fc2_bias,
        fc1_bias,
        qv_bias.reshape(-1),
    )
    packed = lax.all_gather(jnp.concatenate(vectors), "dp", axis=0).astype(jnp.float32)
    wide = []
    at = 0
    for vector in vectors:
        wide.append(packed[:, at : at + vector.shape[0]])
        at += vector.shape[0]
    gain_one, shift_one, gain_two, shift_two, bias_out, bias_fc2, bias_fc1 = (
        part.reshape(-1) for part in wide[:7]
    )
    n_dp = packed.shape[0]
    n_mp = lax.axis_size("mp")
    bias_qv = wide[7].reshape(n_dp, 2, -1).transpose(1, 0, 2).reshape(2, -1)
    seq_rows = tokens.shape[0]
    local_width = w_qkv.shape[2]
    heads_here = local_width // HEAD
    inputs = tokens.astype(jnp.float32)
    normed_one = layer_norm(inputs, gain_one, shift_one).astype(jnp.bfloat16)
    bias_all = jnp.concatenate([bias_qv[0], jnp.zeros_like(bias_qv[0]), bias_qv[1]])
    qkv = (
        jnp.dot(normed_one, whole_qkv, preferred_element_type=jnp.float32) + bias_all
    ).astype(jnp.bfloat16)
    mixed_heads, log_total = attend(qkv, heads_here)
    dp_index = lax.axis_index("dp")
    slot_ids = lax.iota(jnp.int32, counts.shape[0])
    own_count = jnp.sum(jnp.where(slot_ids == dp_index, counts, 0))
    weight_share = own_count.astype(jnp.float32) / jnp.sum(counts).astype(jnp.float32)
    live_rows = lax.iota(jnp.int32, seq_rows) < own_count
    grad_out = jnp.where(live_rows[:, None], cotangent.astype(jnp.float32), 0.0)
    grad_out_low = grad_out.astype(jnp.bfloat16)
    grad_fc2_bias = jnp.sum(grad_out, axis=0) * weight_share
    summed = mix(mixed_heads, whole_out, n_mp, 0)
    act, delta_resid_low, grad_fc1, grad_fc2, two_sums, fc1_sums = ffn(
        tokens,
        summed,
        grad_out_low,
        whole_fc1,
        whole_fc2,
        jnp.stack([gain_two, shift_two, bias_out]),
        bias_fc1[None],
        weight_share.reshape(1, 1),
        n_mp,
        1,
    )
    grad_fc1_bias = fc1_sums[0] * weight_share
    delta_mixed_low = jnp.einsum(
        "sd,cd->sc", delta_resid_low, whole_out, preferred_element_type=jnp.float32
    ).astype(jnp.bfloat16)
    grad_out_proj = (
        jnp.einsum("sc,sd->cd", mixed_heads, delta_resid_low, preferred_element_type=jnp.float32)
        * weight_share
    )
    delta_proj, qv_sums = attend_back(qkv, delta_mixed_low, log_total, heads_here)
    grad_qv = qv_sums.transpose(1, 0, 2).reshape(2, -1) * weight_share
    grad_qkv = (
        jnp.einsum("sd,se->de", normed_one, delta_proj, preferred_element_type=jnp.float32)
        * weight_share
    )
    out_tokens, grad_tokens, one_sums = close(
        delta_proj,
        whole_qkv,
        tokens,
        delta_resid_low,
        summed,
        act,
        whole_fc2,
        jnp.stack([gain_one, bias_out + bias_fc2]),
        n_mp,
        2,
    )
    gain_one_part, shift_one_part = one_sums[0], one_sums[1]
    gain_two_part, shift_two_part, out_bias_part = two_sums[0], two_sums[1], two_sums[2]
    grad_vectors = (
        gain_one_part * weight_share,
        shift_one_part * weight_share,
        gain_two_part * weight_share,
        shift_two_part * weight_share,
        out_bias_part * weight_share,
        grad_fc2_bias,
        grad_fc1_bias,
    )
    stacked = jnp.concatenate(
        [vector.reshape(n_dp, -1) for vector in grad_vectors]
        + [grad_qv.reshape(2, n_dp, -1).transpose(1, 0, 2).reshape(n_dp, -1)],
        axis=1,
    )
    own = lax.psum_scatter(stacked, "dp", scatter_dimension=0, tiled=True)[0]
    pieces = []
    at = 0
    for vector in vectors:
        pieces.append(own[at : at + vector.shape[0]])
        at += vector.shape[0]

    def scatter(grad, axis):
        low = grad.astype(jnp.bfloat16)
        return lax.psum_scatter(low, "dp", scatter_dimension=axis, tiled=True).astype(jnp.float32)

    return (
        out_tokens,
        grad_tokens.astype(jnp.float32),
        scatter(grad_qkv, 0).reshape(w_qkv.shape),
        scatter(grad_out_proj, 1),
        scatter(grad_fc1, 0),
        scatter(grad_fc2, 1),
        pieces[0],
        pieces[1],
        pieces[2],
        pieces[3],
        pieces[7].reshape(2, -1),
        pieces[4],
        pieces[6],
        pieces[5],
    )


def solution(mesh):
    placed = (
        P("dp", None),
        P("dp", None),
        P(),
        P("dp", None, "mp"),
        P("mp", "dp"),
        P("dp", "mp"),
        P("mp", "dp"),
        P("dp"),
        P("dp"),
        P("dp"),
        P("dp"),
        P(None, ("mp", "dp")),
        P("dp"),
        P(("mp", "dp")),
        P("dp"),
    )
    return jax.shard_map(
        shards,
        mesh=mesh,
        in_specs=placed,
        out_specs=(
            P("dp", None),
            P("dp", None),
            P("dp", None, "mp"),
            P("mp", "dp"),
            P("dp", "mp"),
            P("mp", "dp"),
            P("dp"),
            P("dp"),
            P("dp"),
            P("dp"),
            P(None, ("mp", "dp")),
            P("dp"),
            P(("mp", "dp")),
            P("dp"),
        ),
        check_vma=False,
    )
```

```python
import functools
import math

import jax
import jax.numpy as jnp
from jax import lax
from jax.experimental import pallas as pl
from jax.experimental.pallas import tpu as pltpu
from jax.sharding import PartitionSpec as P

HEAD = 128
QROWS = 256
BLOCKS = 8
SUB = 2
VMEM_ALL = 67043328
MESH = pl.DeviceIdType.MESH


EPS = 1e-05
NEG = -1e30


def layer_norm(values, gain_vec, shift_vec):
    center = values - jnp.mean(values, axis=-1, keepdims=True)
    spread = jnp.mean(center * center, axis=-1, keepdims=True)
    return center * lax.rsqrt(spread + EPS) * gain_vec + shift_vec


def future_mask(start, width, rows):
    keys = lax.broadcasted_iota(jnp.int32, (width, rows), 0)
    return keys > start + lax.broadcasted_iota(jnp.int32, (width, rows), 1)

def attend_kernel(inv_root, q_ref, k_ref, v_ref, mixed_ref, lse_ref):
    seq = q_ref.shape[0]
    for start in range(0, seq, QROWS):
        width = start + QROWS
        scores = lax.dot_general(k_ref[:width], q_ref[start:width], (((1,), (1,)), ((), ())),
            preferred_element_type=jnp.float32) * inv_root
        scores = jnp.where(future_mask(start, width, QROWS), NEG, scores)
        peak = jnp.max(scores, axis=0, keepdims=True)
        terms = jnp.exp(scores - peak)
        total = jnp.sum(terms, axis=0, keepdims=True)
        lse_ref[0, :, start:width] = peak + jnp.log(total)
        prob = (terms / total).astype(jnp.bfloat16)
        mixed = lax.dot_general(v_ref[:width], prob, (((0,), (0,)), ((), ())), preferred_element_type=jnp.float32)
        mixed_ref[start:width] = mixed.T.astype(jnp.bfloat16)

def attend(qkv, heads):
    seq = qkv.shape[0]
    col = lambda c: pl.BlockSpec((seq, HEAD), lambda h, c=c: (0, c * heads + h))
    return pl.pallas_call(
        functools.partial(attend_kernel, 1.0 / math.sqrt(HEAD)),
        grid=(heads,), in_specs=[col(0), col(1), col(2)],
        out_specs=[pl.BlockSpec((seq, HEAD), lambda h: (0, h)), pl.BlockSpec((1, 1, seq), lambda h: (h, 0, 0))],
        out_shape=[jax.ShapeDtypeStruct((seq, heads * HEAD), jnp.bfloat16), jax.ShapeDtypeStruct((heads, 1, seq), jnp.float32)],
        name="attend")(qkv, qkv, qkv)

def attend_back_kernel(inv_root, heads, q_ref, k_ref, v_ref, g_ref, lse_ref, out_ref, sums_ref, dk_acc, dv_acc):
    seq = q_ref.shape[0]
    head = pl.program_id(0)
    dk_acc[...] = jnp.zeros_like(dk_acc)
    dv_acc[...] = jnp.zeros_like(dv_acc)
    cols = [pl.ds(pl.multiple_of((c * heads + head) * HEAD, HEAD), HEAD) for c in range(3)]
    dq_sum = jnp.zeros((1, HEAD), jnp.float32)
    for start in range(0, seq, QROWS):
        width = start + QROWS
        q = q_ref[start:width]
        g = g_ref[start:width]
        k = k_ref[:width]
        nt = (((1,), (1,)), ((), ()))
        scores = lax.dot_general(k, q, nt, preferred_element_type=jnp.float32) * inv_root
        scores = jnp.where(future_mask(start, width, QROWS), NEG, scores)
        prob = jnp.exp(scores - lse_ref[0, :, start:width])
        dprob = lax.dot_general(v_ref[:width], g, nt, preferred_element_type=jnp.float32)
        ds = (prob * (dprob - jnp.sum(prob * dprob, axis=0, keepdims=True))).astype(jnp.bfloat16)
        dv_acc[:width] += jnp.dot(prob.astype(jnp.bfloat16), g, preferred_element_type=jnp.float32)
        dk_acc[:width] += jnp.dot(ds, q, preferred_element_type=jnp.float32)
        dq = lax.dot_general(k, ds, (((0,), (0,)), ((), ())), preferred_element_type=jnp.float32).T * inv_root
        out_ref[start:width, cols[0]] = dq.astype(jnp.bfloat16)
        dq_sum += jnp.sum(dq, axis=0, keepdims=True)
    out_ref[:, cols[1]] = (dk_acc[...] * inv_root).astype(jnp.bfloat16)
    dv = dv_acc[...]
    out_ref[:, cols[2]] = dv.astype(jnp.bfloat16)
    sums_ref[0, 0:1] = dq_sum
    sums_ref[0, 1:2] = jnp.sum(dv, axis=0, keepdims=True)

def attend_back(qkv, grad, lse, heads):
    seq = qkv.shape[0]
    col = lambda c: pl.BlockSpec((seq, HEAD), lambda h, c=c: (0, c * heads + h))
    return pl.pallas_call(
        functools.partial(attend_back_kernel, 1.0 / math.sqrt(HEAD), heads),
        grid=(heads,), in_specs=[col(0), col(1), col(2), col(0), pl.BlockSpec((1, 1, seq), lambda h: (h, 0, 0))],
        out_specs=[pl.BlockSpec((seq, 3 * heads * HEAD), lambda h: (0, 0)), pl.BlockSpec((1, 2, HEAD), lambda h: (h, 0, 0))],
        out_shape=[jax.ShapeDtypeStruct((seq, 3 * heads * HEAD), jnp.bfloat16), jax.ShapeDtypeStruct((heads, 2, HEAD), jnp.float32)],
        scratch_shapes=[pltpu.VMEM((seq, HEAD), jnp.float32)] * 2, name="attend_back")(qkv, qkv, qkv, grad, lse)


NN = (((1,), (0,)), ((), ()))
NT = (((1,), (1,)), ((), ()))
GELU_A = math.sqrt(2.0 / math.pi)
GELU_B = 0.044715


def mat(left, right, dims):
    return lax.dot_general(left, right, dims, preferred_element_type=jnp.float32)


class Chain:
    def __init__(self, n, rows, part, held, total, sems):
        self.n, self.part, self.held, self.total = n, part, held, total
        self.s1, self.r1, self.s2, self.r2 = sems
        self.rows = rows // (2 * BLOCKS)
        self.me = lax.axis_index("mp")
        self.last = n - 1
        self.right = lax.rem(self.me + 1, n)
        self.left = lax.rem(self.me + n - 1, n)
        self.sides = (
            (0, self.me, self.right, self.left),
            (1, self.last - self.me, self.left, self.right),
        )
        self.steps = BLOCKS + 2 * self.last

    def start_row(self, half, b):
        return pl.multiple_of(
            ((b // SUB) * 2 * SUB + half * SUB + b % SUB) * self.rows, self.rows
        )

    def cut(self, half, b):
        return pl.ds(self.start_row(half, b), self.rows)

    def forward(self, half, b, src, target):
        return pltpu.make_async_remote_copy(
            src_ref=src.at[self.cut(half, b)],
            dst_ref=self.held.at[self.cut(half, b)],
            send_sem=self.s1.at[half * BLOCKS + b],
            recv_sem=self.r1.at[half * BLOCKS + b],
            device_id={"mp": target},
            device_id_type=MESH,
        )

    def back(self, half, b, target):
        return pltpu.make_async_remote_copy(
            src_ref=self.total.at[self.cut(half, b)],
            dst_ref=self.total.at[self.cut(half, b)],
            send_sem=self.s2.at[half * BLOCKS + b],
            recv_sem=self.r2.at[half * BLOCKS + b],
            device_id={"mp": target},
            device_id_type=MESH,
        )

    def step(self, t, arrived=None):
        for half, pos, ahead, behind in self.sides:
            b = t - pos
            live = jnp.logical_and(b >= 0, b < BLOCKS)

            @pl.when(jnp.logical_and(live, pos == 0))
            def _():
                self.forward(half, b, self.part, ahead).start()

            @pl.when(jnp.logical_and(live, pos > 0))
            def _():
                self.forward(half, b, self.part, ahead).wait_recv()
                cut = self.cut(half, b)
                both = self.held[cut].astype(jnp.float32) + self.part[cut].astype(jnp.float32)

                @pl.when(pos < self.last)
                def _():
                    self.held[cut] = both.astype(jnp.bfloat16)
                    self.forward(half, b, self.held, ahead).start()

                @pl.when(pos == self.last)
                def _():
                    self.total[cut] = both.astype(jnp.bfloat16)
                    self.back(half, b, behind).start()
                    if arrived is not None:
                        arrived(half, b, cut)

        for half, pos, ahead, behind in self.sides:
            b = t - (2 * self.last - pos)
            live = jnp.logical_and(b >= 0, b < BLOCKS)

            @pl.when(jnp.logical_and(live, pos < self.last))
            def _():
                self.back(half, b, behind).wait_recv()

                @pl.when(pos > 0)
                def _():
                    self.back(half, b, behind).start()

                if arrived is not None:
                    arrived(half, b, self.cut(half, b))

    def drain(self):
        def one(b, carry):
            for half, pos, ahead, behind in self.sides:

                @pl.when(pos == 0)
                def _():
                    self.forward(half, b, self.part, ahead).wait_send()

                @pl.when(jnp.logical_and(pos > 0, pos < self.last))
                def _():
                    self.forward(half, b, self.held, ahead).wait_send()

                @pl.when(pos > 0)
                def _():
                    self.back(half, b, behind).wait_send()

            return carry

        lax.fori_loop(0, BLOCKS, one, 0)


def chain_sems():
    return [pltpu.SemaphoreType.DMA((2 * BLOCKS,))] * 4


def greet(n):
    me = lax.axis_index("mp")
    barrier = pltpu.get_barrier_semaphore()

    @pl.when(me > 0)
    def _():
        pl.semaphore_signal(
            barrier, inc=1, device_id={"mp": lax.rem(me + n - 1, n)}, device_id_type=MESH
        )

    @pl.when(me < n - 1)
    def _():
        pl.semaphore_signal(barrier, inc=1, device_id={"mp": lax.rem(me + 1, n)}, device_id_type=MESH)

    pl.semaphore_wait(barrier, jnp.where(me > 0, 1, 0) + jnp.where(me < n - 1, 1, 0))


def moments(wide):
    center = wide - jnp.mean(wide, axis=-1, keepdims=True)
    scale = lax.rsqrt(jnp.mean(center * center, axis=-1, keepdims=True) + EPS)
    return center * scale, scale


def ffn_kernel(
    n, tok_hbm, att_hbm, g_hbm, w1_hbm, w2_hbm, vec_ref, b1_ref, share_ref,
    act_hbm, low_hbm, g1_hbm, g2_hbm, sums_ref, b1sum_ref,
    tok, att, g, w1, w2, act, dpre, nrm, part, held, total, stage, flip,
    in_sem, w_sem, out_sem, stage_sem, s1, r1, s2, r2,
):
    rows, d = tok.shape
    f = w1.shape[1]
    group = 2 * SUB * rows // (2 * BLOCKS)
    groups = rows // group
    tile = 512
    chain = Chain(n, rows, part, held, total, (s1, r1, s2, r2))
    small = chain.rows

    def load(src, dst, which, c):
        cut = pl.ds(pl.multiple_of(c * group, group), group)
        return pltpu.make_async_copy(src.at[cut], dst.at[cut], in_sem.at[which * groups + c])

    def load_group(c):
        load(tok_hbm, tok, 0, c).start()
        load(att_hbm, att, 1, c).start()
        load(g_hbm, g, 2, c).start()

    load_group(0)
    first_weight = pltpu.make_async_copy(w1_hbm, w1, w_sem.at[0])
    second_weight = pltpu.make_async_copy(w2_hbm, w2, w_sem.at[1])
    first_weight.start()
    second_weight.start()
    for c in range(1, groups):
        load_group(c)
    greet(n)
    sums_ref[...] = jnp.zeros_like(sums_ref)
    b1sum_ref[...] = jnp.zeros_like(b1sum_ref)
    gain = vec_ref[0:1]
    shift = vec_ref[1:2]
    out_bias = vec_ref[2:3]

    def act_out(c):
        cut = pl.ds(pl.multiple_of(c * group, group), group)
        return pltpu.make_async_copy(act.at[cut], act_hbm.at[cut], out_sem.at[c])

    def low_out(half, b):
        cut = chain.cut(half, b)
        return pltpu.make_async_copy(att.at[cut], low_hbm.at[cut], out_sem.at[groups + half * BLOCKS + b])

    def compute(c):
        load(tok_hbm, tok, 0, c).wait()
        load(att_hbm, att, 1, c).wait()

        def norm(i, carry):
            cut = pl.ds(pl.multiple_of(c * group + i * small, small), small)
            wide = tok[cut].astype(jnp.float32) + att[cut].astype(jnp.float32) + out_bias
            normal, _ = moments(wide)
            nrm[cut] = (normal * gain + shift).astype(jnp.bfloat16)
            return carry

        lax.fori_loop(0, group // small, norm, 0)
        load(g_hbm, g, 2, c).wait()

    def hidden(c):
        cut = pl.ds(pl.multiple_of(c * group, group), group)

        def one(j, carry):
            cols = pl.ds(pl.multiple_of(j * tile, tile), tile)
            pre = mat(nrm[cut], w1[:, cols], NN) + b1_ref[:, cols]
            square = pre * pre
            bend = jnp.tanh(GELU_A * (pre + GELU_B * (square * pre)))
            half_gate = 0.5 * (1.0 + bend)
            act[cut, cols] = (pre * half_gate).astype(jnp.bfloat16)
            slope = half_gate + 0.5 * pre * (1.0 - bend * bend) * (
                GELU_A * (1.0 + 3.0 * GELU_B * square)
            )
            delta = mat(g[cut], w2[cols, :], NT) * slope
            b1sum_ref[:, cols] += jnp.sum(delta, axis=0, keepdims=True)
            dpre[cut, cols] = delta.astype(jnp.bfloat16)
            return carry

        lax.fori_loop(0, f // tile, one, 0)
        act_out(c).start()

        def two(j, carry):
            cols = pl.ds(pl.multiple_of(j * tile, tile), tile)
            part[cut, cols] = mat(dpre[cut], w1[cols, :], NT).astype(jnp.bfloat16)
            return carry

        lax.fori_loop(0, d // tile, two, 0)

    def arrived(half, b, cut):
        wide = tok[cut].astype(jnp.float32) + att[cut].astype(jnp.float32) + out_bias
        normal, scale = moments(wide)
        delta = total[cut].astype(jnp.float32)
        dn = delta * gain
        inner = dn - jnp.mean(dn, axis=-1, keepdims=True)
        inner = inner - normal * jnp.mean(dn * normal, axis=-1, keepdims=True)
        whole = g[cut].astype(jnp.float32) + scale * inner
        att[cut] = whole.astype(jnp.bfloat16)
        low_out(half, b).start()
        sums_ref[0:1] += jnp.sum(delta * normal, axis=0, keepdims=True)
        sums_ref[1:2] += jnp.sum(delta, axis=0, keepdims=True)
        sums_ref[2:3] += jnp.sum(whole, axis=0, keepdims=True)

    def group_step(c, carry):
        compute(c)

        @pl.when(c == 0)
        def _():
            first_weight.wait()
            second_weight.wait()

        hidden(c)
        for k in range(SUB):
            chain.step(SUB * c + k, arrived)
        return carry

    lax.fori_loop(0, groups, group_step, 0)

    share = share_ref[0, 0]
    side = 256
    tiles_one, tiles_two = d // side, f // side
    count = tiles_one + tiles_two

    def stage_out(i):
        slot = i % 2

        def one():
            return pltpu.make_async_copy(
                stage.at[slot, :, pl.ds(0, f)],
                g1_hbm.at[pl.ds(pl.multiple_of(i * side, side), side)],
                stage_sem.at[slot],
            )

        def two():
            return pltpu.make_async_copy(
                stage.at[slot, :, pl.ds(0, d)],
                g2_hbm.at[pl.ds(pl.multiple_of((i - tiles_one) * side, side), side)],
                stage_sem.at[slot],
            )

        return one, two

    def wait_stage(i):
        one, two = stage_out(i)

        @pl.when(i < tiles_one)
        def _():
            one().wait()

        @pl.when(i >= tiles_one)
        def _():
            two().wait()

    def grads(i):
        slot = i % 2

        @pl.when(i >= 2)
        def _():
            wait_stage(i - 2)

        one, two = stage_out(i)

        def run(left, right, width, at):
            flip[...] = left[:, pl.ds(pl.multiple_of(at * side, side), side)].T

            def tile_of(j, carry):
                cols = pl.ds(pl.multiple_of(j * tile, tile), tile)
                stage[slot, :, cols] = (mat(flip[...], right[:, cols], NN) * share).astype(
                    jnp.bfloat16
                )
                return carry

            lax.fori_loop(0, width // tile, tile_of, 0)

        @pl.when(i < tiles_one)
        def _():
            run(nrm, dpre, f, i)
            one().start()

        @pl.when(i >= tiles_one)
        def _():
            run(act, g, d, i - tiles_one)
            two().start()

    extra = 2 * (n - 1)
    each = -(-count // extra)

    def tail(t, carry):
        for k in range(each):
            i = t * each + k

            @pl.when(i < count)
            def _():
                grads(i)

        chain.step(BLOCKS + t, arrived)
        return carry

    lax.fori_loop(0, extra, tail, 0)
    chain.drain()
    for i in (count - 2, count - 1):
        wait_stage(i)

    def settle(b, carry):
        for half in (0, 1):
            low_out(half, b).wait()
        return carry

    lax.fori_loop(0, BLOCKS, settle, 0)
    for c in range(groups):
        act_out(c).wait()


def ffn(tokens, summed, grad_low, whole_fc1, whole_fc2, vectors, bias_fc1, share, n, cid):
    rows, d = tokens.shape
    f = whole_fc1.shape[1]
    groups = BLOCKS // SUB
    anywhere = pl.BlockSpec(memory_space=pl.ANY)
    vm = pl.BlockSpec(memory_space=pltpu.VMEM)
    low = lambda *shape: pltpu.VMEM(shape, jnp.bfloat16)
    return pl.pallas_call(
        functools.partial(ffn_kernel, n),
        out_shape=[
            jax.ShapeDtypeStruct((rows, f), jnp.bfloat16),
            jax.ShapeDtypeStruct((rows, d), jnp.bfloat16),
            jax.ShapeDtypeStruct((d, f), jnp.bfloat16),
            jax.ShapeDtypeStruct((f, d), jnp.bfloat16),
            jax.ShapeDtypeStruct((3, d), jnp.float32),
            jax.ShapeDtypeStruct((1, f), jnp.float32),
        ],
        in_specs=[anywhere] * 5 + [vm, vm, pl.BlockSpec(memory_space=pltpu.SMEM)],
        out_specs=[anywhere] * 4 + [vm, vm],
        scratch_shapes=[
            low(rows, d), low(rows, d), low(rows, d), low(d, f), low(f, d),
            low(rows, f), low(rows, f), low(rows, d), low(rows, d), low(rows, d), low(rows, d),
            low(2, 256, max(d, f)), low(256, rows),
            pltpu.SemaphoreType.DMA((3 * groups,)),
            pltpu.SemaphoreType.DMA((2,)),
            pltpu.SemaphoreType.DMA((groups + 2 * BLOCKS,)),
            pltpu.SemaphoreType.DMA((2,)),
        ] + chain_sems(),
        compiler_params=pltpu.CompilerParams(
            collective_id=cid, has_side_effects=True, vmem_limit_bytes=VMEM_ALL
        ),
        name="ffn",
    )(tokens, summed, grad_low, whole_fc1, whole_fc2, vectors, bias_fc1, share)


def mix_kernel(n, mixed_ref, w_ref, total, part, held, s1, r1, s2, r2):
    rows = mixed_ref.shape[0]
    group = SUB * rows // BLOCKS
    chain = Chain(n, rows, part, held, total, (s1, r1, s2, r2))
    greet(n)

    def group_step(c, carry):
        cut = pl.ds(pl.multiple_of(c * group, group), group)
        part[cut] = mat(mixed_ref[cut], w_ref[...], NN).astype(jnp.bfloat16)
        for k in range(SUB):
            chain.step(SUB * c + k)
        return carry

    lax.fori_loop(0, rows // group, group_step, 0)
    lax.fori_loop(BLOCKS, chain.steps, lambda t, carry: (chain.step(t), carry)[1], 0)
    chain.drain()


def mix(mixed, whole_out, n, cid):
    rows, d = mixed.shape[0], whole_out.shape[1]
    vm = pl.BlockSpec(memory_space=pltpu.VMEM)
    return pl.pallas_call(
        functools.partial(mix_kernel, n),
        out_shape=jax.ShapeDtypeStruct((rows, d), jnp.bfloat16),
        in_specs=[vm, vm],
        out_specs=vm,
        scratch_shapes=[pltpu.VMEM((rows, d), jnp.bfloat16)] * 2 + chain_sems(),
        compiler_params=pltpu.CompilerParams(
            collective_id=cid, has_side_effects=True, vmem_limit_bytes=28 << 20
        ),
        name="mix",
    )(mixed, whole_out)


def close_kernel(
    n, dproj_hbm, wq_hbm, tok_hbm, low_hbm, att_hbm, act_hbm, w2_hbm, vec_ref,
    out_hbm, gtok_hbm, sums_ref,
    dproj, wq, tok, low, att, act, w2, part_one, held_one, total_one, part_two, held_two, total_two,
    in_sem, out_sem, s1, r1, s2, r2, s3, r3, s4, r4,
):
    rows, d = tok.shape
    f = w2.shape[0]
    group = SUB * rows // BLOCKS
    tile = 512
    one = Chain(n, rows, part_one, held_one, total_one, (s1, r1, s2, r2))
    two = Chain(n, rows, part_two, held_two, total_two, (s3, r3, s4, r4))
    pairs = (
        (dproj_hbm, dproj), (wq_hbm, wq), (act_hbm, act), (w2_hbm, w2),
        (tok_hbm, tok), (att_hbm, att), (low_hbm, low),
    )
    loads = [pltpu.make_async_copy(a, b, in_sem.at[i]) for i, (a, b) in enumerate(pairs)]
    for copy in loads:
        copy.start()
    greet(n)
    sums_ref[...] = jnp.zeros_like(sums_ref)
    gain = vec_ref[0:1]
    me = lax.axis_index("mp")
    head_flag = jnp.where(me == 0, 1.0, 0.0)
    tail_flag = jnp.where(me == n - 1, 1.0, 0.0)

    def one_out(half, b):
        cut = one.cut(half, b)
        return pltpu.make_async_copy(low.at[cut], gtok_hbm.at[cut], out_sem.at[half * BLOCKS + b])

    def two_out(half, b):
        cut = two.cut(half, b)
        return pltpu.make_async_copy(
            total_two.at[cut], out_hbm.at[cut], out_sem.at[(2 + half) * BLOCKS + b]
        )

    def arrived_one(half, b, cut):
        normal, scale = moments(tok[cut].astype(jnp.float32))
        delta = total_one[cut].astype(jnp.float32)
        dn = delta * gain
        inner = dn - jnp.mean(dn, axis=-1, keepdims=True)
        inner = inner - normal * jnp.mean(dn * normal, axis=-1, keepdims=True)
        low[cut] = (low[cut].astype(jnp.float32) + scale * inner).astype(jnp.bfloat16)
        one_out(half, b).start()
        sums_ref[0:1] += jnp.sum(delta * normal, axis=0, keepdims=True)
        sums_ref[1:2] += jnp.sum(delta, axis=0, keepdims=True)

    def arrived_two(half, b, cut):
        two_out(half, b).start()

    def group_step(c, carry):
        cut = pl.ds(pl.multiple_of(c * group, group), group)

        @pl.when(c == 0)
        def _():
            loads[0].wait()
            loads[1].wait()

        def first(j, carry):
            cols = pl.ds(pl.multiple_of(j * tile, tile), tile)
            part_one[cut, cols] = mat(dproj[cut], wq[cols, :], NT).astype(jnp.bfloat16)
            return carry

        lax.fori_loop(0, d // tile, first, 0)

        @pl.when(c == 0)
        def _():
            for copy in loads[2:]:
                copy.wait()

        one.step(SUB * c, arrived_one)
        half_rows = group // 2

        def second(j, carry):
            cols = pl.ds(pl.multiple_of(j * tile, tile), tile)
            for half, flag in ((0, head_flag), (1, tail_flag)):
                own = pl.ds(pl.multiple_of(c * group + half * half_rows, half_rows), half_rows)
                wide = tok[own, cols].astype(jnp.float32) + att[own, cols].astype(jnp.float32)
                part = mat(act[own], w2[:, cols], NN) + flag * (wide + vec_ref[1:2, cols])
                part_two[own, cols] = part.astype(jnp.bfloat16)
            return carry

        lax.fori_loop(0, d // tile, second, 0)
        for k in range(1, SUB):
            one.step(SUB * c + k, arrived_one)
        return carry

    lax.fori_loop(0, rows // group, group_step, 0)

    def later(t, carry):
        one.step(t, arrived_one)
        two.step(t - BLOCKS, arrived_two)
        return carry

    lax.fori_loop(BLOCKS, one.steps + BLOCKS, later, 0)
    one.drain()
    two.drain()

    def settle(b, carry):
        for half in (0, 1):
            one_out(half, b).wait()
            two_out(half, b).wait()
        return carry

    lax.fori_loop(0, BLOCKS, settle, 0)


def close(dproj, whole_qkv, tokens, low, summed, act, whole_fc2, vectors, n, cid):
    rows, d = tokens.shape
    anywhere = pl.BlockSpec(memory_space=pl.ANY)
    vm = pl.BlockSpec(memory_space=pltpu.VMEM)
    held = [pltpu.VMEM((rows, d), jnp.bfloat16)]
    like = lambda x: pltpu.VMEM(x.shape, jnp.bfloat16)
    return pl.pallas_call(
        functools.partial(close_kernel, n),
        out_shape=[
            jax.ShapeDtypeStruct((rows, d), jnp.bfloat16),
            jax.ShapeDtypeStruct((rows, d), jnp.bfloat16),
            jax.ShapeDtypeStruct((2, d), jnp.float32),
        ],
        in_specs=[anywhere] * 7 + [vm],
        out_specs=[anywhere] * 2 + [vm],
        scratch_shapes=[like(dproj), like(whole_qkv)] + held * 3 + [like(act), like(whole_fc2)]
        + held * 6
        + [pltpu.SemaphoreType.DMA((7,)), pltpu.SemaphoreType.DMA((4 * BLOCKS,))]
        + chain_sems() + chain_sems(),
        compiler_params=pltpu.CompilerParams(
            collective_id=cid, has_side_effects=True, vmem_limit_bytes=VMEM_ALL
        ),
        name="close",
    )(dproj, whole_qkv, tokens, low, summed, act, whole_fc2, vectors)


def greet_all(axis, n):
    me = lax.axis_index(axis)
    barrier = pltpu.get_barrier_semaphore()
    for offset in range(1, n):
        pl.semaphore_signal(
            barrier, inc=1, device_id={axis: lax.rem(me + offset, n)}, device_id_type=MESH
        )
    pl.semaphore_wait(barrier, n - 1)


def spread_kernel(n, x_ref, out_ref, got, send, recv):
    me = lax.axis_index("dp")
    greet_all("dp", n)

    def copy(offset):
        target = lax.rem(me + offset, n)
        return pltpu.make_async_remote_copy(
            src_ref=x_ref.at[target],
            dst_ref=got.at[offset - 1],
            send_sem=send.at[offset - 1],
            recv_sem=recv.at[offset - 1],
            device_id={"dp": target},
            device_id_type=MESH,
        )

    for offset in range(1, n):
        copy(offset).start()
    total = x_ref[me]
    for offset in range(1, n):
        copy(offset).wait()
        total = total + got[offset - 1]
    out_ref[...] = total


def spread(x, n, cid):
    vm = pl.BlockSpec(memory_space=pltpu.VMEM)
    return pl.pallas_call(
        functools.partial(spread_kernel, n),
        out_shape=jax.ShapeDtypeStruct(x.shape[1:], x.dtype),
        in_specs=[vm],
        out_specs=vm,
        scratch_shapes=[
            pltpu.VMEM((n - 1,) + x.shape[1:], x.dtype),
            pltpu.SemaphoreType.DMA((n - 1,)),
            pltpu.SemaphoreType.DMA((n - 1,)),
        ],
        compiler_params=pltpu.CompilerParams(
            collective_id=cid, has_side_effects=True, vmem_limit_bytes=8 << 20
        ),
        name="spread",
    )(x)


def open_kernel(
    n, width, own_hbm, small_ref, tok_hbm,
    whole_hbm, nrm_hbm, qkv_hbm, packed_ref,
    whole, tok, nrm, acc, qkv, vec, bias,
    load_sem, out_sem, small_send, small_recv, send, recv,
):
    me = lax.axis_index("dp")
    rows, d = tok.shape
    wide = whole.shape[1]
    shard = d // n
    half = shard // 2
    core = lax.rem(me, 2)
    partner = me + 1 - 2 * core
    along_x = me + 2 - 4 * lax.rem(me // 2, 2)
    along_y = me + 4 - 8 * (me // 4)
    across = along_x + along_y - me
    partner_x = along_x + 1 - 2 * core
    partner_y = along_y + 1 - 2 * core
    partner_across = across + 1 - 2 * core

    def piece(owner, h):
        return pl.ds(pl.multiple_of(owner * shard + h * half, half), half)

    def copy(kind, h, src, owner, target):
        return pltpu.make_async_remote_copy(
            src_ref=src,
            dst_ref=whole.at[piece(owner, h)],
            send_sem=send.at[kind * 2 + h],
            recv_sem=recv.at[kind * 2 + h],
            device_id={"dp": target},
            device_id_type=MESH,
        )

    def own(kind, h, target):
        return copy(kind, h, own_hbm.at[pl.ds(h * half, half)], me, target)

    def relay(kind, h, owner, target):
        return copy(kind, h, whole.at[piece(owner, h)], owner, target)

    def arrive(kind, h, owner):
        copy(kind, h, whole.at[piece(owner, h)], owner, partner).wait_recv()

    def small_copy(offset, slot=me):
        return pltpu.make_async_remote_copy(
            src_ref=small_ref,
            dst_ref=packed_ref.at[slot],
            send_sem=small_send.at[offset - 1],
            recv_sem=small_recv.at[offset - 1],
            device_id={"dp": lax.rem(me + offset, n)},
            device_id_type=MESH,
        )

    tok_load = pltpu.make_async_copy(tok_hbm, tok, load_sem.at[0])
    tok_load.start()
    own_load = pltpu.make_async_copy(
        own_hbm, whole.at[pl.ds(pl.multiple_of(me * shard, shard), shard)], load_sem.at[1]
    )
    own_load.start()
    greet_all("dp", n)
    for offset in range(1, n):
        small_copy(offset).start()
    sends = [
        own(0, 0, along_x), own(1, 1, along_y), own(0, 1, along_x), own(1, 0, along_y),
        own(2, 0, partner), own(2, 1, partner),
    ]
    for item in sends:
        item.start()
    packed_ref[me] = small_ref[...]
    for offset in range(1, n):
        small_copy(offset, lax.rem(me + n - offset, n)).wait_recv()
    lanes = shard // HEAD
    for s in range(n):
        for which in range(2):
            for k in range(lanes):
                at = s * shard + k * HEAD
                vec[which : which + 1, at : at + HEAD] = packed_ref[
                    s, which * lanes + k : which * lanes + k + 1
                ].astype(jnp.float32)
    local = wide // 3
    rise = lax.broadcasted_iota(jnp.int32, (HEAD, local), 0)
    run = lax.broadcasted_iota(jnp.int32, (HEAD, local), 1)
    base = small_ref.shape[0] - 2
    bias[...] = jnp.zeros_like(bias)
    for s in range(n):
        place = jnp.where(jnp.logical_and(run == s * width + rise, rise < width), 1.0, 0.0)
        got = mat(packed_ref[s, base : base + 2], place.astype(jnp.bfloat16), NN)
        bias[0:1, 0:local] += got[0:1]
        bias[0:1, 2 * local : 3 * local] += got[1:2]
    tok_load.wait()
    small = 64

    def norm(i, carry):
        cut = pl.ds(pl.multiple_of(i * small, small), small)
        normal, _ = moments(tok[cut].astype(jnp.float32))
        nrm[cut] = (normal * vec[0:1] + vec[1:2]).astype(jnp.bfloat16)
        return carry

    lax.fori_loop(0, rows // small, norm, 0)
    nrm_out = pltpu.make_async_copy(nrm, nrm_hbm, out_sem.at[0])
    nrm_out.start()
    relays = []

    def pass_on(kind, h, owner, target):
        item = relay(kind, h, owner, target)
        item.start()
        relays.append(item)

    arrive(0, 0, along_x)
    pass_on(3, 0, along_x, along_y)
    pass_on(4, 0, along_x, partner)
    arrive(1, 1, along_y)
    pass_on(3, 1, along_y, along_x)
    pass_on(5, 1, along_y, partner)
    arrive(0, 1, along_x)
    pass_on(4, 1, along_x, partner)
    arrive(1, 0, along_y)
    pass_on(5, 0, along_y, partner)
    own_load.wait()
    for h in (0, 1):
        arrive(2, h, partner)
        arrive(4, h, partner_x)
        arrive(5, h, partner_y)
    tall = rows // 2
    tile = local
    near = (me, partner, along_x, along_y, partner_x, partner_y)

    def product_at(owners, r, cols):
        cut = pl.ds(pl.multiple_of(r * tall, tall), tall)
        total = None
        for owner in owners:
            at = pl.ds(pl.multiple_of(owner * shard, shard), shard)
            one = mat(nrm[cut, at], whole[at, cols], NN)
            total = one if total is None else total + one
        return total

    def early(i, carry):
        r = i // 3
        cols = pl.ds(pl.multiple_of(lax.rem(i, 3) * tile, tile), tile)
        acc[pl.ds(pl.multiple_of(r * tall, tall), tall), cols] = product_at(near, r, cols)
        return carry

    lax.fori_loop(0, 6, early, 0)
    for h in (0, 1):
        arrive(3, h, across)
        pass_on(6, h, across, partner)
    for h in (0, 1):
        arrive(6, h, partner_across)
    whole_out = pltpu.make_async_copy(whole, whole_hbm, out_sem.at[1])
    whole_out.start()

    def late(i, carry):
        r = i // 3
        cut = pl.ds(pl.multiple_of(r * tall, tall), tall)
        cols = pl.ds(pl.multiple_of(lax.rem(i, 3) * tile, tile), tile)
        total = acc[cut, cols] + product_at((across, partner_across), r, cols)
        qkv[cut, cols] = (total + bias[0:1, cols]).astype(jnp.bfloat16)
        return carry

    lax.fori_loop(0, 6, late, 0)
    qkv_out = pltpu.make_async_copy(qkv, qkv_hbm, out_sem.at[2])
    qkv_out.start()
    for item in sends + relays:
        item.wait_send()
    for offset in range(1, n):
        small_copy(offset).wait_send()
    nrm_out.wait()
    whole_out.wait()
    qkv_out.wait()


def open_layer(own, small, tokens, width, n, cid):
    rows, d = tokens.shape
    wide = own.shape[1]
    anywhere = pl.BlockSpec(memory_space=pl.ANY)
    vm = pl.BlockSpec(memory_space=pltpu.VMEM)
    low = lambda *shape: pltpu.VMEM(shape, jnp.bfloat16)
    full = lambda *shape: pltpu.VMEM(shape, jnp.float32)
    return pl.pallas_call(
        functools.partial(open_kernel, n, width),
        out_shape=[
            jax.ShapeDtypeStruct((d, wide), jnp.bfloat16),
            jax.ShapeDtypeStruct((rows, d), jnp.bfloat16),
            jax.ShapeDtypeStruct((rows, wide), jnp.bfloat16),
            jax.ShapeDtypeStruct((n,) + small.shape, jnp.bfloat16),
        ],
        in_specs=[anywhere, vm, anywhere],
        out_specs=[anywhere] * 3 + [vm],
        scratch_shapes=[
            low(d, wide), low(rows, d), low(rows, d), full(rows, wide), low(rows, wide),
            full(2, d), full(1, wide),
            pltpu.SemaphoreType.DMA((2,)),
            pltpu.SemaphoreType.DMA((3,)),
            pltpu.SemaphoreType.DMA((n - 1,)),
            pltpu.SemaphoreType.DMA((n - 1,)),
            pltpu.SemaphoreType.DMA((14,)),
            pltpu.SemaphoreType.DMA((14,)),
        ],
        compiler_params=pltpu.CompilerParams(
            collective_id=cid, has_side_effects=True, vmem_limit_bytes=40 << 20
        ),
        name="open",
    )(own, small, tokens)


def shards(
    tokens,
    cotangent,
    counts,
    w_qkv,
    w_out,
    w_fc1,
    w_fc2,
    ln1_gain,
    ln1_bias,
    ln2_gain,
    ln2_bias,
    qv_bias,
    out_bias,
    fc1_bias,
    fc2_bias,
):
    whole_out = lax.all_gather(w_out, "dp", axis=1, tiled=True)
    whole_fc1 = lax.all_gather(w_fc1, "dp", axis=0, tiled=True)
    whole_fc2 = lax.all_gather(w_fc2, "dp", axis=1, tiled=True)
    vectors = (
        ln1_gain,
        ln1_bias,
        ln2_gain,
        ln2_bias,
        out_bias,
        fc2_bias,
        fc1_bias,
        qv_bias.reshape(-1),
    )
    n_dp = lax.axis_size("dp")
    own_qkv = w_qkv.reshape(w_qkv.shape[0], -1)
    fused = n_dp == 8 and w_qkv.shape[0] % (2 * HEAD) == 0
    width = qv_bias.shape[1]
    if fused:
        lines = []
        for vector in vectors[:7]:
            lines.append(vector.reshape(-1, HEAD))
        lines.append(jnp.pad(qv_bias, ((0, 0), (0, HEAD - width))))
        whole_qkv, normed_one, qkv, gathered = open_layer(
            own_qkv, jnp.concatenate(lines), tokens, width, n_dp, 4
        )
        flat = gathered.astype(jnp.float32).reshape(n_dp, -1)
        packed = jnp.concatenate(
            [flat[:, : -2 * HEAD], flat[:, -2 * HEAD : width - 2 * HEAD], flat[:, -HEAD : width - HEAD]],
            axis=1,
        )
    else:
        whole_qkv = lax.all_gather(own_qkv, "dp", axis=0, tiled=True)
        packed = lax.all_gather(jnp.concatenate(vectors), "dp", axis=0).astype(jnp.float32)
    wide = []
    at = 0
    for vector in vectors:
        wide.append(packed[:, at : at + vector.shape[0]])
        at += vector.shape[0]
    gain_one, shift_one, gain_two, shift_two, bias_out, bias_fc2, bias_fc1 = (
        part.reshape(-1) for part in wide[:7]
    )
    n_mp = lax.axis_size("mp")
    bias_qv = wide[7].reshape(n_dp, 2, -1).transpose(1, 0, 2).reshape(2, -1)
    seq_rows = tokens.shape[0]
    local_width = w_qkv.shape[2]
    heads_here = local_width // HEAD
    if not fused:
        inputs = tokens.astype(jnp.float32)
        normed_one = layer_norm(inputs, gain_one, shift_one).astype(jnp.bfloat16)
        bias_all = jnp.concatenate([bias_qv[0], jnp.zeros_like(bias_qv[0]), bias_qv[1]])
        qkv = (
            jnp.dot(normed_one, whole_qkv, preferred_element_type=jnp.float32) + bias_all
        ).astype(jnp.bfloat16)
    mixed_heads, log_total = attend(qkv, heads_here)
    dp_index = lax.axis_index("dp")
    slot_ids = lax.iota(jnp.int32, counts.shape[0])
    own_count = jnp.sum(jnp.where(slot_ids == dp_index, counts, 0))
    weight_share = own_count.astype(jnp.float32) / jnp.sum(counts).astype(jnp.float32)
    live_rows = lax.iota(jnp.int32, seq_rows) < own_count
    grad_out = jnp.where(live_rows[:, None], cotangent.astype(jnp.float32), 0.0)
    grad_out_low = grad_out.astype(jnp.bfloat16)
    grad_fc2_bias = jnp.sum(grad_out, axis=0) * weight_share
    summed = mix(mixed_heads, whole_out, n_mp, 0)
    act, delta_resid_low, grad_fc1, grad_fc2, two_sums, fc1_sums = ffn(
        tokens,
        summed,
        grad_out_low,
        whole_fc1,
        whole_fc2,
        jnp.stack([gain_two, shift_two, bias_out]),
        bias_fc1[None],
        weight_share.reshape(1, 1),
        n_mp,
        1,
    )
    grad_fc1_bias = fc1_sums[0] * weight_share
    delta_mixed_low = jnp.einsum(
        "sd,cd->sc", delta_resid_low, whole_out, preferred_element_type=jnp.float32
    ).astype(jnp.bfloat16)
    grad_out_proj = (
        jnp.einsum("sc,sd->cd", mixed_heads, delta_resid_low, preferred_element_type=jnp.float32)
        * weight_share
    )
    delta_proj, qv_sums = attend_back(qkv, delta_mixed_low, log_total, heads_here)
    grad_qv = qv_sums.transpose(1, 0, 2).reshape(2, -1) * weight_share
    grad_qkv = (
        jnp.einsum("sd,se->de", normed_one, delta_proj, preferred_element_type=jnp.float32)
        * weight_share
    )
    out_tokens, grad_tokens, one_sums = close(
        delta_proj,
        whole_qkv,
        tokens,
        delta_resid_low,
        summed,
        act,
        whole_fc2,
        jnp.stack([gain_one, bias_out + bias_fc2]),
        n_mp,
        2,
    )
    gain_one_part, shift_one_part = one_sums[0], one_sums[1]
    gain_two_part, shift_two_part, out_bias_part = two_sums[0], two_sums[1], two_sums[2]
    grad_vectors = (
        gain_one_part * weight_share,
        shift_one_part * weight_share,
        gain_two_part * weight_share,
        shift_two_part * weight_share,
        out_bias_part * weight_share,
        grad_fc2_bias,
        grad_fc1_bias,
    )
    stacked = jnp.concatenate(
        [vector.reshape(n_dp, -1) for vector in grad_vectors]
        + [grad_qv.reshape(2, n_dp, -1).transpose(1, 0, 2).reshape(n_dp, -1)],
        axis=1,
    )
    length = stacked.shape[1]
    padded = jnp.pad(stacked, ((0, 0), (0, -length % HEAD))).reshape(n_dp, -1, HEAD)
    own = spread(padded, n_dp, 3).reshape(-1)[:length]
    pieces = []
    at = 0
    for vector in vectors:
        pieces.append(own[at : at + vector.shape[0]])
        at += vector.shape[0]

    def scatter(grad, axis):
        low = grad.astype(jnp.bfloat16)
        return lax.psum_scatter(low, "dp", scatter_dimension=axis, tiled=True).astype(jnp.float32)

    return (
        out_tokens,
        grad_tokens.astype(jnp.float32),
        scatter(grad_qkv, 0).reshape(w_qkv.shape),
        scatter(grad_out_proj, 1),
        scatter(grad_fc1, 0),
        scatter(grad_fc2, 1),
        pieces[0],
        pieces[1],
        pieces[2],
        pieces[3],
        pieces[7].reshape(2, -1),
        pieces[4],
        pieces[6],
        pieces[5],
    )


def solution(mesh):
    placed = (
        P("dp", None),
        P("dp", None),
        P(),
        P("dp", None, "mp"),
        P("mp", "dp"),
        P("dp", "mp"),
        P("mp", "dp"),
        P("dp"),
        P("dp"),
        P("dp"),
        P("dp"),
        P(None, ("mp", "dp")),
        P("dp"),
        P(("mp", "dp")),
        P("dp"),
    )
    return jax.shard_map(
        shards,
        mesh=mesh,
        in_specs=placed,
        out_specs=(
            P("dp", None),
            P("dp", None),
            P("dp", None, "mp"),
            P("mp", "dp"),
            P("dp", "mp"),
            P("mp", "dp"),
            P("dp"),
            P("dp"),
            P("dp"),
            P("dp"),
            P(None, ("mp", "dp")),
            P("dp"),
            P(("mp", "dp")),
            P("dp"),
        ),
        check_vma=False,
    )
```
